64 devices in a mesh: dp: 4 (over x, y), tp: 16 (over z, core).
Axes of the slice: x: 2, y: 2, z: 8, core: 2. Of those that a mesh axis runs over, the one named last changes fastest.
The devices are a block of a 4x4x8 slice.
Arguments:
- hidden: bfloat16 [4, 4096, 4096], P('dp', 'tp'), parts along dimension 0
- attn_gain: float32 [4096], replicated
- w_q: bfloat16 [4096, 4096], P(None, 'tp')
- w_k: bfloat16 [4096, 4096], P(None, 'tp')
- w_v: bfloat16 [4096, 4096], P(None, 'tp')
- q_gain: float32 [4096], P('tp')
- k_gain: float32 [4096], P('tp')
- w_o: bfloat16 [4096, 4096], P('tp')
Outputs:
- output 1: bfloat16 [4, 4096, 4096], P('dp', 'tp'), parts along dimension 0
- output 2: bfloat16 [4, 4096, 32, 128], P('dp', None, 'tp'), parts along dimension 0
- output 3: bfloat16 [4, 4096, 32, 128], P('dp', None, 'tp'), parts along dimension 0
There are 4 independent parts. The reference program is written for one: setup_inputs(seed, part) draws one part's arguments, and reference() takes and returns one part's arrays. A program takes and returns all parts, laid end to end along the dimension named above; an argument that names none is the same for every part.
All inputs are finite; a program needn't handle non-finite values.
Results may differ from the reference program's by a relative error of at most 0.0111495.
Values are sent between devices in bfloat16 or wider.
A program may use at most 768 MiB of HBM per device.

```python
import jax
import jax.numpy as jnp
from jax import lax

BATCH_SIZE = 1
SEQ_LEN = 4096
D_MODEL = 4096
N_HEADS = 32
HEAD_DIM = 128


def setup_inputs(seed: int = 0, part: int = 0) -> dict:
    base_key = jax.random.key(seed)
    part_keys = jax.random.split(jax.random.fold_in(base_key, part), 2)
    key_list = jax.random.split(base_key, 9)
    x_noise = jax.random.normal(part_keys[0], (BATCH_SIZE, SEQ_LEN, D_MODEL), jnp.float32)
    x_mean = jax.random.normal(part_keys[1], (BATCH_SIZE, 1, D_MODEL), jnp.float32)
    head_pos = jnp.arange(N_HEADS, dtype=jnp.float32) / max(N_HEADS - 1, 1)
    q_heads = 10.0 ** (head_pos - 0.5) * jax.random.uniform(key_list[0], (N_HEADS,), jnp.float32, 0.8, 1.2)
    k_heads = 10.0 ** (0.5 - head_pos) * jax.random.uniform(key_list[1], (N_HEADS,), jnp.float32, 0.8, 1.2)
    fan_scale = D_MODEL ** -0.5
    w_shape = (D_MODEL, D_MODEL)
    w_q = jax.random.normal(key_list[2], w_shape, jnp.float32) * (fan_scale * jnp.repeat(q_heads, HEAD_DIM))[None, :]
    w_k = jax.random.normal(key_list[3], w_shape, jnp.float32) * (fan_scale * jnp.repeat(k_heads, HEAD_DIM))[None, :]
    w_v = jax.random.normal(key_list[4], w_shape, jnp.float32) * fan_scale
    w_o = jax.random.normal(key_list[5], w_shape, jnp.float32) * fan_scale
    return {
        'hidden': (x_noise + x_mean).astype(jnp.bfloat16),
        'attn_gain': jax.random.uniform(key_list[6], (D_MODEL,), jnp.float32, 0.5, 1.5),
        'w_q': w_q.astype(jnp.bfloat16),
        'w_k': w_k.astype(jnp.bfloat16),
        'w_v': w_v.astype(jnp.bfloat16),
        'q_gain': jax.random.uniform(key_list[7], (D_MODEL,), jnp.float32, 1.5, 3.5),
        'k_gain': jax.random.uniform(key_list[8], (D_MODEL,), jnp.float32, 1.5, 3.5),
        'w_o': w_o.astype(jnp.bfloat16),
    }


def rope_tables(seq_len, head_dim):
    half_dim = head_dim // 2
    inv_freq = 10000.0 ** (-jnp.arange(half_dim, dtype=jnp.float32) * (2.0 / head_dim))
    angles = jnp.arange(seq_len, dtype=jnp.float32)[:, None] * inv_freq[None, :]
    return jnp.cos(angles), jnp.sin(angles)


def apply_rope(heads_in, cos_tab, sin_tab):
    half_dim = heads_in.shape[-1] // 2
    lower_half = heads_in[..., :half_dim]
    upper_half = heads_in[..., half_dim:]
    cos_bcast = cos_tab[None, :, None, :]
    sin_bcast = sin_tab[None, :, None, :]
    return jnp.concatenate([lower_half * cos_bcast - upper_half * sin_bcast, upper_half * cos_bcast + lower_half * sin_bcast], axis=-1)


def reference(hidden, attn_gain, w_q, w_k, w_v, q_gain, k_gain, w_o):
    x_f32 = hidden.astype(jnp.float32)
    inv_rms = lax.rsqrt(jnp.mean(x_f32 * x_f32, axis=-1, keepdims=True) + 1e-5)
    h_rows = (x_f32 * inv_rms * attn_gain).astype(jnp.bfloat16).reshape(BATCH_SIZE * SEQ_LEN, D_MODEL)
    q_raw = jnp.dot(h_rows, w_q, preferred_element_type=jnp.float32).astype(jnp.bfloat16).astype(jnp.float32)
    k_raw = jnp.dot(h_rows, w_k, preferred_element_type=jnp.float32).astype(jnp.bfloat16).astype(jnp.float32)
    v_rows = jnp.dot(h_rows, w_v, preferred_element_type=jnp.float32).astype(jnp.bfloat16)
    q_normed = q_raw * lax.rsqrt(jnp.mean(q_raw * q_raw, axis=-1, keepdims=True) + 1e-5) * q_gain
    k_normed = k_raw * lax.rsqrt(jnp.mean(k_raw * k_raw, axis=-1, keepdims=True) + 1e-5) * k_gain
    cos_tab, sin_tab = rope_tables(SEQ_LEN, HEAD_DIM)
    head_shape = (BATCH_SIZE, SEQ_LEN, N_HEADS, HEAD_DIM)
    q_rot = apply_rope(q_normed.reshape(head_shape), cos_tab, sin_tab).astype(jnp.bfloat16)
    k_rot = apply_rope(k_normed.reshape(head_shape), cos_tab, sin_tab).astype(jnp.bfloat16)
    v_heads = v_rows.reshape(head_shape)
    positions = jnp.arange(SEQ_LEN)
    causal = positions[:, None] >= positions[None, :]
    score_scale = HEAD_DIM ** -0.5

    def one_head(head_args):
        q_head, k_head, v_head = head_args
        scores = jnp.einsum('bqd,bkd->bqk', q_head.astype(jnp.float32), k_head.astype(jnp.float32)) * score_scale
        scores = jnp.where(causal[None], scores, -1e30)
        prob_bf = jax.nn.softmax(scores, axis=-1).astype(jnp.bfloat16)
        head_out = jnp.einsum('bqk,bkd->bqd', prob_bf.astype(jnp.float32), v_head.astype(jnp.float32))
        return head_out.astype(jnp.bfloat16)

    per_head = lax.map(one_head, (jnp.moveaxis(q_rot, 2, 0), jnp.moveaxis(k_rot, 2, 0), jnp.moveaxis(v_heads, 2, 0)))
    attn_rows = jnp.moveaxis(per_head, 0, 2).reshape(BATCH_SIZE * SEQ_LEN, D_MODEL)
    y_rows = jnp.dot(attn_rows, w_o, preferred_element_type=jnp.float32).astype(jnp.bfloat16)
    hidden_out = (x_f32 + y_rows.reshape(hidden.shape).astype(jnp.float32)).astype(jnp.bfloat16)
    return (hidden_out, k_rot, v_heads)
```

```python
import functools
import math

import jax
import jax.numpy as jnp
import numpy as np
from jax import lax
from jax.experimental import pallas as pl
from jax.experimental.pallas import tpu as pltpu
from jax.sharding import PartitionSpec as P

HEAD_DIM = 128
EPS = 1e-5
PIECE = 64
SUM_PIECES = 4
F32 = jnp.float32
BF16 = jnp.bfloat16


def rope_constants(seq_len):
    half = HEAD_DIM // 2
    inv_freq = 10000.0 ** (-np.arange(half) * (2.0 / HEAD_DIM))
    inv_freq = np.concatenate([inv_freq, inv_freq])
    sign = np.concatenate([-np.ones(half), np.ones(half)])
    base = (np.arange(seq_len // PIECE) * PIECE)[:, None] * inv_freq
    off = np.arange(PIECE)[:, None] * inv_freq
    return [jnp.asarray(t, F32) for t in (np.cos(base), sign * np.sin(base), np.cos(off), sign * np.sin(off))]


def block_kernel(
    n, x_hbm, gain, wq_hbm, wk_hbm, wv_hbm, wo_hbm, q_gain, k_gain, cos_b, sin_b, cos_o, sin_o,
    out_hbm, k_hbm, v_hbm,
    hbuf, wqkv, wo, q_s, k_s, v_s, x_s, ybuf, o_s, sq_out, sq_in, inv,
    ld_sem, ag_send, ag_recv, dd_send, dd_recv, sq_send, sq_recv, iv_send, iv_recv,
    rs_send, rs_recv, sb_send, sb_recv, st_sem,
):
    nz = n // 2
    me = lax.axis_index("tp")
    z, c = me // 2, lax.rem(me, 2)
    sib = z * 2 + 1 - c
    n_rows, width = x_s.shape
    half = n_rows // 2
    pieces = half // PIECE
    units = nz * pieces
    cols = q_s.shape[1]
    heads = cols // HEAD_DIM
    sub = half // SUM_PIECES
    k_tile = 2 * n_rows

    def chip(offset):
        return lax.rem(z + offset + 2 * nz, nz)

    def toward(d, hops=1):
        return chip(hops) if d == 0 else chip(-hops)

    def rows(start, size):
        return pl.ds(pl.multiple_of(start, size), size)

    def remote(src, dst, send, recv, dev):
        return pltpu.make_async_remote_copy(
            src_ref=src, dst_ref=dst, send_sem=send, recv_sem=recv,
            device_id={"tp": dev}, device_id_type=pl.DeviceIdType.MESH)

    loads = [pltpu.make_async_copy(x_hbm, x_s, ld_sem.at[0])]
    for i, w in enumerate((wq_hbm, wk_hbm, wv_hbm)):
        loads.append(pltpu.make_async_copy(w, wqkv.at[i], ld_sem.at[1 + i]))
    loads.append(pltpu.make_async_copy(wo_hbm, wo, ld_sem.at[4]))
    for load in loads:
        load.start()

    barrier = pltpu.get_barrier_semaphore()

    def greet(i, _):
        pl.semaphore_signal(barrier, inc=1, device_id={"tp": lax.rem(me + i, n)}, device_id_type=pl.DeviceIdType.MESH)
        return 0

    lax.fori_loop(1, n, greet, 0)

    def quarter(u, d):
        return hbuf.at[u, rows((2 * d + c) * PIECE, PIECE)]

    def ring_copy(u, d):
        return remote(quarter(u, d), quarter(u + pieces, d), ag_send.at[u, d], ag_recv.at[u, d], toward(d) * 2 + c)

    def pair_copy(u, d):
        return remote(quarter(u, d), quarter(u, d), dd_send.at[u, d], dd_recv.at[u, d], sib)

    loads[0].wait()
    for p in range(pieces):
        for d in range(2):
            x = x_s[pl.ds(d * half + p * PIECE, PIECE), :].astype(F32)
            inv_rms = lax.rsqrt(jnp.mean(x * x, axis=-1, keepdims=True) + EPS)
            hbuf[p, rows((2 * d + c) * PIECE, PIECE), :] = (x * inv_rms * gain[...]).astype(BF16)
        if p == 0:
            pl.semaphore_wait(barrier, n - 1)
        for d in range(2):
            ring_copy(p, d).start()
            pair_copy(p, d).start()

    def sq_copy(u, d, p, dev):
        return remote(sq_out.at[u, d], sq_in.at[me, p], sq_send.at[u, d], sq_recv.at[me, p], dev)

    def project(v):
        s, p = v // pieces, lax.rem(v, pieces)
        for d in range(2):
            pair_copy(v, d).wait_recv()

        @pl.when(v == 0)
        def _():
            for load in loads[1:]:
                load.wait()

        h = hbuf[v]
        sums = []
        for i, dst in enumerate((q_s, k_s, v_s)):
            out = jnp.dot(h, wqkv[i], preferred_element_type=F32).astype(BF16)
            for d in range(2):
                src = chip(-s) if d == 0 else chip(s)
                for cc in range(2):
                    at = (2 * src + cc) * n_rows + d * half + p * PIECE
                    lo = (2 * d + cc) * PIECE
                    dst[rows(at, PIECE), :] = out[lo:lo + PIECE]
            if i < 2:
                wide = out.astype(F32)
                sq = wide * wide
                lanes = sq[:, :HEAD_DIM]
                for j in range(1, heads):
                    lanes = lanes + sq[:, j * HEAD_DIM:(j + 1) * HEAD_DIM]
                sums.append(lanes)
        for d in range(2):
            for i in range(2):
                part = sums[i][d * 2 * PIECE:(d + 1) * 2 * PIECE]
                sq_out[v, d, pl.ds(i, 1), :] = jnp.sum(part.T, axis=0, keepdims=True)
            owner = chip(-s - 1) if d == 0 else chip(s + 1)

            @pl.when(s < nz - 1)
            def _(d=d, owner=owner):
                sq_copy(v, d, p, owner * 2 + d).start()

            @pl.when((s == nz - 1) & (c != d))
            def _(d=d):
                sq_copy(v, d, p, sib).start()

            @pl.when((s == nz - 1) & (c == d))
            def _(d=d):
                sq_in[me, p] = sq_out[v, d]

    def gather_step(u, _):
        @pl.when((u >= pieces) & (u < units))
        def _():
            for d in range(2):
                ring_copy(u - pieces, d).wait_recv()

                @pl.when(u < units - pieces)
                def _(d=d):
                    ring_copy(u, d).start()

                pair_copy(u, d).start()

        project(u - 1)
        return 0

    lax.fori_loop(1, units + 1, gather_step, 0)

    v_out = pltpu.make_async_copy(v_s, v_hbm, st_sem.at[0])
    v_out.start()

    def drain_gather(u, _):
        for d in range(2):
            pair_copy(u, d).wait_send()

            @pl.when(u < units - pieces)
            def _(d=d):
                ring_copy(u, d).wait_send()
                sq_copy(u, d, 0, sib).wait_send()

            @pl.when((u >= units - pieces) & (c != d))
            def _(d=d):
                sq_copy(u, d, 0, sib).wait_send()

        return 0

    lax.fori_loop(0, units, drain_gather, 0)

    def sq_arrived(i, _):
        peer = lax.rem(me + i, n)
        for p in range(pieces):
            remote(sq_out.at[0, 0], sq_in.at[peer, p], sq_send.at[0, 0], sq_recv.at[peer, p], sib).wait_recv()
        return 0

    lax.fori_loop(1, n, sq_arrived, 0)
    total = sq_in[0]
    for i in range(1, n):
        total = total + sq_in[i]
    inv[me] = lax.rsqrt(total / (cols * n) + EPS)

    def inv_copy(i):
        dev = lax.rem(me + i, n)
        return remote(inv.at[me], inv.at[me], iv_send.at[i], iv_recv.at[me], dev)

    def inv_start(i, _):
        inv_copy(i).start()
        return 0

    def inv_wait(i, _):
        peer = lax.rem(me + i, n)
        remote(inv.at[peer], inv.at[peer], iv_send.at[i], iv_recv.at[peer], sib).wait_recv()
        return 0

    def inv_sent(i, _):
        inv_copy(i).wait_send()
        return 0

    lax.fori_loop(1, n, inv_start, 0)
    lax.fori_loop(1, n, inv_wait, 0)
    lax.fori_loop(1, n, inv_sent, 0)

    def normed_rope(raw, which, src, d, p):
        own = lax.rem(src + (nz - 1 if d == 0 else 1), nz) * 2 + d
        scale = inv[own, p][which:which + 1]
        scale = jnp.broadcast_to(scale, (HEAD_DIM, HEAD_DIM)).T
        gains = (q_gain, k_gain)[which][...]
        done = []
        for cc in range(2):
            b = (2 * src + cc) * (n_rows // PIECE) + d * pieces + p
            cb, sb = cos_b[pl.ds(b, 1), :], sin_b[pl.ds(b, 1), :]
            cos = cb * cos_o[...] - sb * sin_o[...]
            sin = sb * cos_o[...] + cb * sin_o[...]
            out = []
            for j in range(heads):
                lanes = slice(j * HEAD_DIM, (j + 1) * HEAD_DIM)
                t = raw[cc][:, lanes].astype(F32) * scale[cc * PIECE:(cc + 1) * PIECE] * gains[:, lanes]
                out.append((t * cos + pltpu.roll(t, HEAD_DIM // 2, 1) * sin).astype(BF16))
            done.append(out)
        return done

    def finish_keys(src, _):
        for d in range(2):
            for p in range(pieces):
                at = [rows((2 * src + cc) * n_rows + d * half + p * PIECE, PIECE) for cc in range(2)]
                done = normed_rope([k_s[r, :] for r in at], 1, src, d, p)
                for cc in range(2):
                    for j in range(heads):
                        k_s[at[cc], j * HEAD_DIM:(j + 1) * HEAD_DIM] = done[cc][j]
        return 0

    lax.fori_loop(0, nz, finish_keys, 0)
    k_out = pltpu.make_async_copy(k_s, k_hbm, st_sem.at[1])
    k_out.start()

    scale = HEAD_DIM ** -0.5 * math.log2(math.e)

    def attend(t, d):
        blk = lax.rem(z + 2 * nz - 1 - t, nz) if d == 0 else lax.rem(z + 1 + t, nz)
        parts = [[None] * pieces for _ in range(2)]
        for p in range(pieces):
            at = [rows((2 * blk + cc) * n_rows + d * half + p * PIECE, PIECE) for cc in range(2)]
            done = normed_rope([q_s[r, :] for r in at], 0, blk, d, p)
            for cc in range(2):
                parts[cc][p] = done[cc]
        q = [jnp.concatenate([parts[cc][p][j] for cc in range(2) for p in range(pieces)], axis=0) for j in range(heads)]

        def tile(j, at, m, l, acc, mask):
            lanes = slice(j * HEAD_DIM, (j + 1) * HEAD_DIM)
            sc = lax.dot_general(q[j], k_s[at, lanes], (((1,), (1,)), ((), ())), preferred_element_type=F32) * scale
            if mask is not None:
                sc = jnp.where(mask, sc, -1e30)
            m_new = jnp.maximum(m, jnp.max(sc, axis=1, keepdims=True))
            prob = jnp.exp2(sc - m_new)
            fade = jnp.exp2(m - m_new)
            l = l * fade + jnp.sum(prob, axis=1, keepdims=True)
            acc = acc * fade + jnp.dot(prob.astype(BF16), v_s[at, lanes], preferred_element_type=F32)
            return m_new, l, acc

        def step(i, carry):
            at = rows(i * k_tile, k_tile)
            return tuple(tile(j, at, *carry[j], None) for j in range(heads))

        zero = (jnp.full((n_rows, 1), -1e30, F32), jnp.zeros((n_rows, 1), F32), jnp.zeros((n_rows, HEAD_DIM), F32))
        carry = lax.fori_loop(0, blk, step, (zero,) * heads)
        r = lax.broadcasted_iota(jnp.int32, (n_rows, k_tile), 0)
        col = lax.broadcasted_iota(jnp.int32, (n_rows, k_tile), 1)
        mask = jnp.where(r < half, r, r + (n_rows - half)) + d * half >= col
        at = rows(blk * k_tile, k_tile)
        for j in range(heads):
            _, l, acc = tile(j, at, *carry[j], mask)
            o_s[d, :, j * HEAD_DIM:(j + 1) * HEAD_DIM] = (acc / l).astype(BF16)

    def share_copy(t, d):
        return remote(
            ybuf.at[lax.rem(t, 2), 1 - c, d], hbuf.at[nz * pieces // 2 + t, pl.ds(d * half, half)],
            sb_send.at[t, d], sb_recv.at[t, d], sib)

    y_tile = min(width, 1024)

    def emit(t, d):
        slot = lax.rem(t, 2)

        @pl.when(t >= 2)
        def _():
            share_copy(t - 2, d).wait_send()

        def column(i, _):
            at = rows(i * y_tile, y_tile)
            y = jnp.dot(o_s[d], wo[:, at], preferred_element_type=F32).astype(BF16)
            ybuf[slot, 0, d, :, at] = y[:half]
            ybuf[slot, 1, d, :, at] = y[half:]
            return 0

        lax.fori_loop(0, width // y_tile, column, 0)
        share_copy(t, d).start()

    def sum_copy(s, d, k):
        at = rows(d * half + k * sub, sub)
        return remote(hbuf.at[s, at], hbuf.at[s + 1, at], rs_send.at[s, d * SUM_PIECES + k],
                      rs_recv.at[s, d * SUM_PIECES + k], toward(d) * 2 + c)

    def out_copy(d, k):
        at = rows(d * half + k * sub, sub)
        return pltpu.make_async_copy(hbuf.at[nz - 1, at], out_hbm.at[at], st_sem.at[2 + d * SUM_PIECES + k])

    def add_up(s, k):
        for d in range(2):
            if k == 0:
                share_copy(s, d).wait_recv()

            @pl.when(s >= 1)
            def _(d=d):
                sum_copy(s - 1, d, k).wait_recv()

            at = rows(d * half + k * sub, sub)

            def column(i, _, d=d, at=at):
                lanes = rows(i * y_tile, y_tile)
                y = ybuf[lax.rem(s, 2), c, d, pl.ds(k * sub, sub), lanes].astype(F32)
                y = y + hbuf[nz * pieces // 2 + s, at, lanes].astype(F32)
                run = hbuf[s, at, lanes].astype(F32)
                y = (y + jnp.where(s >= 1, run, 0.0)).astype(BF16)
                hbuf[s, at, lanes] = y

                @pl.when(s == nz - 1)
                def _():
                    hbuf[s, at, lanes] = (x_s[at, lanes].astype(F32) + y.astype(F32)).astype(BF16)

                return 0

            lax.fori_loop(0, width // y_tile, column, 0)

            @pl.when(s < nz - 1)
            def _(d=d):
                sum_copy(s, d, k).start()

            @pl.when(s == nz - 1)
            def _(d=d):
                out_copy(d, k).start()

    def scatter_step(t, _):
        for k in range(SUM_PIECES):
            @pl.when(t >= 1)
            def _(k=k):
                add_up(t - 1, k)

            @pl.when(t < nz)
            def _(k=k):
                if k % 2 == 0:
                    attend(t, k // 2)
                else:
                    emit(t, k // 2)

        return 0

    lax.fori_loop(0, nz + 1, scatter_step, 0)

    def drain_scatter(s, _):
        for d in range(2):
            for k in range(SUM_PIECES):
                sum_copy(s, d, k).wait_send()
        return 0

    lax.fori_loop(0, nz - 1, drain_scatter, 0)
    for d in range(2):
        for t in (nz - 2, nz - 1):
            share_copy(t, d).wait_send()
        for k in range(SUM_PIECES):
            out_copy(d, k).wait()
    v_out.wait()
    k_out.wait()


def solution(mesh):
    n = mesh.shape["tp"]

    def local_block(x_local, attn_gain, wq, wk, wv, q_gain, k_gain, wo):
        _, n_rows, width = x_local.shape
        cols = wq.shape[1]
        seq_len = n * n_rows
        nz, pieces = n // 2, n_rows // 2 // PIECE
        units = nz * pieces
        tables = rope_constants(seq_len)
        any_spec = pl.BlockSpec(memory_space=pl.ANY)
        vmem_spec = pl.BlockSpec(memory_space=pltpu.VMEM)
        dma = pltpu.SemaphoreType.DMA
        out, k_rot, v_rows = pl.pallas_call(
            functools.partial(block_kernel, n),
            out_shape=(
                jax.ShapeDtypeStruct((n_rows, width), BF16),
                jax.ShapeDtypeStruct((seq_len, cols), BF16),
                jax.ShapeDtypeStruct((seq_len, cols), BF16),
            ),
            in_specs=[any_spec, vmem_spec] + [any_spec] * 4 + [vmem_spec] * 6,
            out_specs=(any_spec,) * 3,
            scratch_shapes=[
                pltpu.VMEM((units, 4 * PIECE, width), BF16),
                pltpu.VMEM((3, width, cols), BF16),
                pltpu.VMEM((cols, width), BF16),
                pltpu.VMEM((seq_len, cols), BF16),
                pltpu.VMEM((seq_len, cols), BF16),
                pltpu.VMEM((seq_len, cols), BF16),
                pltpu.VMEM((n_rows, width), BF16),
                pltpu.VMEM((2, 2, 2, n_rows // 2, width), BF16),
                pltpu.VMEM((2, n_rows, cols), BF16),
                pltpu.VMEM((units, 2, 2, 2 * PIECE), F32),
                pltpu.VMEM((n, pieces, 2, 2 * PIECE), F32),
                pltpu.VMEM((n, pieces, 2, 2 * PIECE), F32),
                dma((5,)),
                dma((units, 2)), dma((units, 2)), dma((units, 2)), dma((units, 2)),
                dma((units, 2)), dma((n, pieces)), dma((n,)), dma((n,)),
                dma((nz - 1, 2 * SUM_PIECES)), dma((nz - 1, 2 * SUM_PIECES)),
                dma((nz, 2)), dma((nz, 2)), dma((2 + 2 * SUM_PIECES,)),
            ],
            compiler_params=pltpu.CompilerParams(
                collective_id=0, has_side_effects=True, vmem_limit_bytes=67043328),
            name="attention_block",
        )(x_local[0], attn_gain[None], wq, wk, wv, wo, q_gain[None], k_gain[None], *tables)
        head_shape = (1, seq_len, cols // HEAD_DIM, HEAD_DIM)
        return out[None], k_rot.reshape(head_shape), v_rows.reshape(head_shape)

    seq_spec = P("dp", "tp", None)
    head_spec = P("dp", None, "tp", None)
    col_spec = P(None, "tp")
    return jax.shard_map(
        local_block, mesh=mesh,
        in_specs=(seq_spec, P(None), col_spec, col_spec, col_spec, P("tp"), P("tp"), P("tp", None)),
        out_specs=(seq_spec, head_spec, head_spec), check_vma=False)
```

```python
import functools
import math

import jax
import jax.numpy as jnp
import numpy as np
from jax import lax
from jax.experimental import pallas as pl
from jax.experimental.pallas import tpu as pltpu
from jax.sharding import PartitionSpec as P

HEAD_DIM = 128
EPS = 1e-5
PIECE = 64
SUM_PIECES = 4
F32 = jnp.float32
BF16 = jnp.bfloat16


def rope_constants(seq_len):
    half = HEAD_DIM // 2
    inv_freq = 10000.0 ** (-np.arange(half) * (2.0 / HEAD_DIM))
    inv_freq = np.concatenate([inv_freq, inv_freq])
    sign = np.concatenate([-np.ones(half), np.ones(half)])
    base = (np.arange(seq_len // PIECE) * PIECE)[:, None] * inv_freq
    off = np.arange(PIECE)[:, None] * inv_freq
    return [jnp.asarray(t, F32) for t in (np.cos(base), sign * np.sin(base), np.cos(off), sign * np.sin(off))]


def block_kernel(
    n, x_hbm, gain, wq_hbm, wk_hbm, wv_hbm, wo_hbm, q_gain, k_gain, cos_b, sin_b, cos_o, sin_o,
    out_hbm, k_hbm, v_hbm,
    hbuf, wqkv, wo, q_s, k_f, k_s, v_s, v_t, ybuf, o_s, kv_st, sq_out, sq_in, inv,
    ld_sem, ag_send, ag_recv, dd_send, dd_recv, sq_send, sq_recv, iv_send, iv_recv,
    rs_send, rs_recv, sb_send, sb_recv, st_sem, out_sem,
):
    nz = n // 2
    me = lax.axis_index("tp")
    z, c = me // 2, lax.rem(me, 2)
    sib = z * 2 + 1 - c
    n_rows, width = x_hbm.shape
    half = n_rows // 2
    pieces = half // PIECE
    units = nz * pieces
    cols = q_s.shape[1]
    heads = cols // HEAD_DIM
    sub = half // SUM_PIECES
    k_tile = 2 * n_rows
    shares = units // 2
    cast_rows = q_s.shape[0] // (nz * SUM_PIECES)

    def chip(offset):
        return lax.rem(z + offset + 2 * nz, nz)

    def toward(d, hops=1):
        return chip(hops) if d == 0 else chip(-hops)

    def rows(start, size):
        return pl.ds(pl.multiple_of(start, size), size)

    def remote(src, dst, send, recv, dev):
        return pltpu.make_async_remote_copy(
            src_ref=src, dst_ref=dst, send_sem=send, recv_sem=recv,
            device_id={"tp": dev}, device_id_type=pl.DeviceIdType.MESH)

    def x_load(d, p):
        at = pl.ds(d * half + p * PIECE, PIECE)
        return pltpu.make_async_copy(x_hbm.at[at], ybuf.at[0, d, pl.ds(p * PIECE, PIECE)], ld_sem.at[4 + d * pieces + p])

    for p in range(pieces):
        for d in range(2):
            x_load(d, p).start()
    loads = [pltpu.make_async_copy(w, wqkv.at[i], ld_sem.at[i]) for i, w in enumerate((wq_hbm, wk_hbm, wv_hbm))]
    loads.append(pltpu.make_async_copy(wo_hbm, wo, ld_sem.at[3]))

    barrier = pltpu.get_barrier_semaphore()

    def greet(i, _):
        pl.semaphore_signal(barrier, inc=1, device_id={"tp": lax.rem(me + i, n)}, device_id_type=pl.DeviceIdType.MESH)
        return 0

    lax.fori_loop(1, n, greet, 0)

    def quarter(u, d):
        return hbuf.at[u, rows((2 * d + c) * PIECE, PIECE)]

    def ring_copy(u, d):
        return remote(quarter(u, d), quarter(u + pieces, d), ag_send.at[u, d], ag_recv.at[u, d], toward(d) * 2 + c)

    def pair_copy(u, d):
        return remote(quarter(u, d), quarter(u, d), dd_send.at[u, d], dd_recv.at[u, d], sib)

    for p in range(pieces):
        for d in range(2):
            x_load(d, p).wait()
            x = ybuf[0, d, pl.ds(p * PIECE, PIECE), :].astype(F32)
            inv_rms = lax.rsqrt(jnp.mean(x * x, axis=-1, keepdims=True) + EPS)
            hbuf[p, rows((2 * d + c) * PIECE, PIECE), :] = (x * inv_rms * gain[...]).astype(BF16)
        if p == 0:
            for load in loads:
                load.start()
            pl.semaphore_wait(barrier, n - 1)
        for d in range(2):
            ring_copy(p, d).start()
            pair_copy(p, d).start()

    def sq_copy(u, d, p, dev):
        return remote(sq_out.at[u, d], sq_in.at[me, p], sq_send.at[u, d], sq_recv.at[me, p], dev)

    def rotate(t, src, d, cc, p):
        b = (2 * src + cc) * (n_rows // PIECE) + d * pieces + p
        cb, sb = cos_b[pl.ds(b, 1), :], sin_b[pl.ds(b, 1), :]
        cos = cb * cos_o[...] - sb * sin_o[...]
        sin = sb * cos_o[...] + cb * sin_o[...]
        heads_in = [t[:, j * HEAD_DIM:(j + 1) * HEAD_DIM] for j in range(heads)]
        return [x * cos + pltpu.roll(x, HEAD_DIM // 2, 1) * sin for x in heads_in]

    def project(v):
        s, p = v // pieces, lax.rem(v, pieces)
        for d in range(2):
            pair_copy(v, d).wait_recv()

        @pl.when(v == 0)
        def _():
            for load in loads:
                load.wait()

        h = hbuf[v]
        parts = [(d, cc, chip(-s) if d == 0 else chip(s), (2 * d + cc) * PIECE) for d in range(2) for cc in range(2)]

        def at(d, cc, src):
            return rows((2 * src + cc) * n_rows + d * half + p * PIECE, PIECE)

        outs, sums = [], []
        for i in range(2):
            out = jnp.dot(h, wqkv[i], preferred_element_type=F32).astype(BF16)
            wide = out.astype(F32)
            sq = wide * wide
            lanes = sq[:, :HEAD_DIM]
            for j in range(1, heads):
                lanes = lanes + sq[:, j * HEAD_DIM:(j + 1) * HEAD_DIM]
            outs.append(out)
            sums.append(lanes)
        for d, cc, src, lo in parts:
            q_s[at(d, cc, src), :] = outs[0][lo:lo + PIECE]
            k_f[at(d, cc, src), :] = outs[1][lo:lo + PIECE].astype(F32)
        for d in range(2):
            for i in range(2):
                part = sums[i][d * 2 * PIECE:(d + 1) * 2 * PIECE]
                sq_out[v, d, pl.ds(i, 1), :] = jnp.sum(part.T, axis=0, keepdims=True)
            owner = chip(-s - 1) if d == 0 else chip(s + 1)

            @pl.when(s < nz - 1)
            def _(d=d, owner=owner):
                sq_copy(v, d, p, owner * 2 + d).start()

            @pl.when((s == nz - 1) & (c != d))
            def _(d=d):
                sq_copy(v, d, p, sib).start()

            @pl.when((s == nz - 1) & (c == d))
            def _(d=d):
                sq_in[me, p] = sq_out[v, d]

    def project_rest(v):
        s, p = v // pieces, lax.rem(v, pieces)
        out = jnp.dot(hbuf[v], wqkv[2], preferred_element_type=F32).astype(BF16)
        for d in range(2):
            src = chip(-s) if d == 0 else chip(s)
            for cc in range(2):
                at = rows((2 * src + cc) * n_rows + d * half + p * PIECE, PIECE)
                lo = (2 * d + cc) * PIECE
                v_s[at, :] = out[lo:lo + PIECE]
                done = rotate(k_f[at, :] * k_gain[...], src, d, cc, p)
                for j in range(heads):
                    k_f[at, j * HEAD_DIM:(j + 1) * HEAD_DIM] = done[j]

    def drain(u):
        for d in range(2):
            pair_copy(u, d).wait_send()

            @pl.when(u < units - pieces)
            def _(d=d):
                ring_copy(u, d).wait_send()

            @pl.when((u < units - pieces) | (c != d))
            def _(d=d):
                sq_copy(u, d, 0, sib).wait_send()

    def gather_step(u, _):
        @pl.when(u >= pieces)
        def _():
            for d in range(2):
                ring_copy(u - pieces, d).wait_recv()

                @pl.when(u < units - pieces)
                def _(d=d):
                    ring_copy(u, d).start()

                pair_copy(u, d).start()

        project(u)

        @pl.when(u >= 2)
        def _():
            drain(u - 2)

        @pl.when(u < units - 1)
        def _():
            project_rest(u)

        return 0

    lax.fori_loop(0, units, gather_step, 0)
    drain(units - 2)
    drain(units - 1)

    def sq_arrived(i, _):
        peer = lax.rem(me + i, n)
        for p in range(pieces):
            remote(sq_out.at[0, 0], sq_in.at[peer, p], sq_send.at[0, 0], sq_recv.at[peer, p], sib).wait_recv()
        return 0

    lax.fori_loop(1, n, sq_arrived, 0)
    total = sq_in[0]
    for i in range(1, n):
        total = total + sq_in[i]
    inv[me] = lax.rsqrt(total / (cols * n) + EPS)

    def inv_copy(i):
        dev = lax.rem(me + i, n)
        return remote(inv.at[me], inv.at[me], iv_send.at[i], iv_recv.at[me], dev)

    def inv_start(i, _):
        inv_copy(i).start()
        return 0

    def inv_wait(i, _):
        peer = lax.rem(me + i, n)
        remote(inv.at[peer], inv.at[peer], iv_send.at[i], iv_recv.at[peer], sib).wait_recv()
        return 0

    def inv_sent(i, _):
        inv_copy(i).wait_send()
        return 0

    lax.fori_loop(1, n, inv_start, 0)
    project_rest(units - 1)

    def turn_values(i, _):
        at = rows(i * k_tile, k_tile)
        v_t[:, at] = v_s[at, :].T
        return 0

    lax.fori_loop(0, q_s.shape[0] // k_tile, turn_values, 0)
    lax.fori_loop(1, n, inv_wait, 0)
    lax.fori_loop(1, n, inv_sent, 0)

    def row_scale(which, src, d, p):
        own = lax.rem(src + (nz - 1 if d == 0 else 1), nz) * 2 + d
        return jnp.broadcast_to(inv[own, p][which:which + 1], (HEAD_DIM, HEAD_DIM)).T

    def piece_rows(src, cc, d, p):
        return rows((2 * src + cc) * n_rows + d * half + p * PIECE, PIECE)

    def finish_keys(src, _):
        for d in range(2):
            for p in range(pieces):
                scale = row_scale(1, src, d, p)
                for cc in range(2):
                    at = piece_rows(src, cc, d, p)
                    for j in range(heads):
                        lanes = slice(j * HEAD_DIM, (j + 1) * HEAD_DIM)
                        k_s[at, lanes] = (k_f[at, lanes] * scale[cc * PIECE:(cc + 1) * PIECE]).astype(BF16)
        return 0

    lax.fori_loop(0, nz, finish_keys, 0)

    scale = HEAD_DIM ** -0.5 * math.log2(math.e)

    queries = 2 * PIECE

    def attend(t, d, p):
        blk = lax.rem(z + 2 * nz - 1 - t, nz) if d == 0 else lax.rem(z + 1 + t, nz)
        factor = row_scale(0, blk, d, p)
        factor = jnp.concatenate([factor] * heads, axis=1)
        parts = []
        for cc in range(2):
            raw = q_s[piece_rows(blk, cc, d, p), :].astype(F32)
            parts.append(rotate(raw * factor[cc * PIECE:(cc + 1) * PIECE] * q_gain[...], blk, d, cc, p))
        q_t = [jnp.concatenate([parts[0][j], parts[1][j]], axis=0).T.astype(BF16) for j in range(heads)]

        def tile(at, carry, mask):
            lanes = [slice(j * HEAD_DIM, (j + 1) * HEAD_DIM) for j in range(heads)]
            score = [jnp.dot(k_s[at, lanes[j]], q_t[j], preferred_element_type=F32) for j in range(heads)]
            if mask is not None:
                score = [jnp.where(mask, sc, -1e30) for sc in score]
            peak = [jnp.maximum(carry[j][0], jnp.max(score[j], axis=0, keepdims=True)) for j in range(heads)]
            prob = [jnp.exp2(score[j] * scale - peak[j] * scale) for j in range(heads)]
            fade = [jnp.exp2((carry[j][0] - peak[j]) * scale) for j in range(heads)]
            acc = [jnp.dot(v_t[lanes[j], at], prob[j].astype(BF16), preferred_element_type=F32) for j in range(heads)]
            return tuple(
                (peak[j], carry[j][1] * fade[j] + jnp.sum(prob[j], axis=0, keepdims=True), carry[j][2] * fade[j] + acc[j])
                for j in range(heads))

        zero = (jnp.full((1, queries), -1e30, F32), jnp.zeros((1, queries), F32), jnp.zeros((HEAD_DIM, queries), F32))
        carry = lax.fori_loop(0, blk, lambda i, kept: tile(rows(i * k_tile, k_tile), kept, None), (zero,) * heads)
        key = lax.broadcasted_iota(jnp.int32, (k_tile, queries), 0)
        r = lax.broadcasted_iota(jnp.int32, (k_tile, queries), 1)
        mask = jnp.where(r < PIECE, r, r + (n_rows - PIECE)) + (d * half + p * PIECE) >= key
        carry = tile(rows(blk * k_tile, k_tile), carry, mask)
        for j in range(heads):
            _, l, acc = carry[j]
            o_s[:, j * HEAD_DIM:(j + 1) * HEAD_DIM] = (acc / l).T.astype(BF16)

    def share_copy(t, d, p):
        return remote(
            ybuf.at[1, d, pl.ds(p * PIECE, PIECE)], hbuf.at[shares + t, pl.ds(d * half + p * PIECE, PIECE)],
            sb_send.at[t, d * pieces + p], sb_recv.at[t, d * pieces + p], sib)

    y_tile = min(width, 1024)

    def emit(t, d, p):
        @pl.when(t >= 1)
        def _():
            share_copy(t - 1, d, p).wait_send()

        def column(i, _):
            at = rows(i * y_tile, y_tile)
            y = jnp.dot(o_s[...], wo[:, at], preferred_element_type=F32).astype(BF16)
            for cc in range(2):
                ybuf[cc + c - 2 * cc * c, d, pl.ds(p * PIECE, PIECE), at] = y[cc * PIECE:(cc + 1) * PIECE]
            return 0

        lax.fori_loop(0, width // y_tile, column, 0)
        share_copy(t, d, p).start()

    def sum_copy(s, d, k):
        at = rows(d * half + k * sub, sub)
        return remote(hbuf.at[s, at], hbuf.at[s + 1, at], rs_send.at[s, d * SUM_PIECES + k],
                      rs_recv.at[s, d * SUM_PIECES + k], toward(d) * 2 + c)

    def out_copy(d, k):
        at = rows(d * half + k * sub, sub)
        return pltpu.make_async_copy(hbuf.at[nz - 1, at], out_hbm.at[at], out_sem.at[d * SUM_PIECES + k])

    def add_up(s, k):
        for d in range(2):
            if k * sub % PIECE == 0:
                share_copy(s, d, k * sub // PIECE).wait_recv()

            @pl.when(s >= 1)
            def _(d=d):
                sum_copy(s - 1, d, k).wait_recv()

            at = rows(d * half + k * sub, sub)

            def column(i, _, d=d, at=at):
                lanes = rows(i * y_tile, y_tile)
                y = ybuf[0, d, pl.ds(k * sub, sub), lanes].astype(F32)
                y = y + hbuf[shares + s, at, lanes].astype(F32)
                run = hbuf[s, at, lanes].astype(F32)
                y = (y + jnp.where(s >= 1, run, 0.0)).astype(BF16)
                hbuf[s, at, lanes] = y

                @pl.when(s == nz - 1)
                def _():
                    hbuf[s, at, lanes] = (hbuf[shares, at, lanes].astype(F32) + y.astype(F32)).astype(BF16)

                return 0

            lax.fori_loop(0, width // y_tile, column, 0)

            @pl.when(s < nz - 1)
            def _(d=d):
                sum_copy(s, d, k).start()

            @pl.when(s == nz - 1)
            def _(d=d):
                out_copy(d, k).start()

    x_again = pltpu.make_async_copy(x_hbm, hbuf.at[shares], ld_sem.at[0])

    def cache_copy(i, which):
        at = rows(i * cast_rows, cast_rows)
        return pltpu.make_async_copy(
            kv_st.at[which, lax.rem(i, 2)], (k_hbm, v_hbm)[which].at[at], st_sem.at[which, lax.rem(i, 2)])

    def write_caches(i):
        for which in range(2):
            @pl.when(i >= 2)
            def _(which=which):
                cache_copy(i - 2, which).wait()

            part = (k_s, v_s)[which][rows(i * cast_rows, cast_rows), :]
            kv_st[which, lax.rem(i, 2)] = part.reshape(cast_rows, heads, HEAD_DIM)
            cache_copy(i, which).start()

    def scatter_step(t, _):
        @pl.when(t == 2)
        def _():
            x_again.start()

        @pl.when(t == nz)
        def _():
            x_again.wait()

        for k in range(SUM_PIECES):
            @pl.when(t >= 1)
            def _(k=k):
                write_caches((t - 1) * SUM_PIECES + k)
                add_up(t - 1, k)

            d, late = k % 2, k < 2

            @pl.when((t >= 1) if late else (t < nz))
            def _(d=d, late=late):
                attend(t - late, d, int(late))
                emit(t - late, d, int(late))

        return 0

    lax.fori_loop(0, nz + 1, scatter_step, 0)

    def drain_scatter(s, _):
        for d in range(2):
            for k in range(SUM_PIECES):
                sum_copy(s, d, k).wait_send()
        return 0

    lax.fori_loop(0, nz - 1, drain_scatter, 0)
    for d in range(2):
        for p in range(pieces):
            share_copy(nz - 1, d, p).wait_send()
        for k in range(SUM_PIECES):
            out_copy(d, k).wait()
    for i in (nz * SUM_PIECES - 2, nz * SUM_PIECES - 1):
        for which in range(2):
            cache_copy(i, which).wait()


def solution(mesh):
    n = mesh.shape["tp"]

    def local_block(x_local, attn_gain, wq, wk, wv, q_gain, k_gain, wo):
        _, n_rows, width = x_local.shape
        cols = wq.shape[1]
        seq_len = n * n_rows
        nz, pieces = n // 2, n_rows // 2 // PIECE
        units = nz * pieces
        tables = rope_constants(seq_len)
        any_spec = pl.BlockSpec(memory_space=pl.ANY)
        vmem_spec = pl.BlockSpec(memory_space=pltpu.VMEM)
        dma = pltpu.SemaphoreType.DMA
        out, k_rot, v_rows = pl.pallas_call(
            functools.partial(block_kernel, n),
            out_shape=(
                jax.ShapeDtypeStruct((n_rows, width), BF16),
                jax.ShapeDtypeStruct((seq_len, cols // HEAD_DIM, HEAD_DIM), BF16),
                jax.ShapeDtypeStruct((seq_len, cols // HEAD_DIM, HEAD_DIM), BF16),
            ),
            in_specs=[any_spec, vmem_spec] + [any_spec] * 4 + [vmem_spec] * 6,
            out_specs=(any_spec,) * 3,
            scratch_shapes=[
                pltpu.VMEM((units, 4 * PIECE, width), BF16),
                pltpu.VMEM((3, width, cols), BF16),
                pltpu.VMEM((cols, width), BF16),
                pltpu.VMEM((seq_len, cols), BF16),
                pltpu.VMEM((seq_len, cols), F32),
                pltpu.VMEM((seq_len, cols), BF16),
                pltpu.VMEM((seq_len, cols), BF16),
                pltpu.VMEM((cols, seq_len), BF16),
                pltpu.VMEM((2, 2, n_rows // 2, width), BF16),
                pltpu.VMEM((2 * PIECE, cols), BF16),
                pltpu.VMEM((2, 2, seq_len // (nz * SUM_PIECES), cols // HEAD_DIM, HEAD_DIM), BF16),
                pltpu.VMEM((units, 2, 2, 2 * PIECE), F32),
                pltpu.VMEM((n, pieces, 2, 2 * PIECE), F32),
                pltpu.VMEM((n, pieces, 2, 2 * PIECE), F32),
                dma((4 + 2 * pieces,)),
                dma((units, 2)), dma((units, 2)), dma((units, 2)), dma((units, 2)),
                dma((units, 2)), dma((n, pieces)), dma((n,)), dma((n,)),
                dma((nz - 1, 2 * SUM_PIECES)), dma((nz - 1, 2 * SUM_PIECES)),
                dma((nz, 2 * pieces)), dma((nz, 2 * pieces)), dma((2, 2)), dma((2 * SUM_PIECES,)),
            ],
            compiler_params=pltpu.CompilerParams(
                collective_id=0, has_side_effects=True, vmem_limit_bytes=67043328),
            name="attention_block",
        )(x_local[0], attn_gain[None], wq, wk, wv, wo, q_gain[None], k_gain[None], *tables)
        return out[None], k_rot[None], v_rows[None]

    seq_spec = P("dp", "tp", None)
    head_spec = P("dp", None, "tp", None)
    col_spec = P(None, "tp")
    return jax.shard_map(
        local_block, mesh=mesh,
        in_specs=(seq_spec, P(None), col_spec, col_spec, col_spec, P("tp"), P("tp"), P("tp", None)),
        out_specs=(seq_spec, head_spec, head_spec), check_vma=False)
```

```python
import functools
import math

import jax
import jax.numpy as jnp
import numpy as np
from jax import lax
from jax.experimental import pallas as pl
from jax.experimental.pallas import tpu as pltpu
from jax.sharding import PartitionSpec as P

HEAD_DIM = 128
EPS = 1e-5
PIECE = 64
SUM_PIECES = 4
KERNEL_VMEM = 60700000
FLUSH_PARTS = 4
F32 = jnp.float32
BF16 = jnp.bfloat16


def rope_constants(seq_len):
    half = HEAD_DIM // 2
    inv_freq = 10000.0 ** (-np.arange(half) * (2.0 / HEAD_DIM))
    inv_freq = np.concatenate([inv_freq, inv_freq])
    sign = np.concatenate([-np.ones(half), np.ones(half)])
    base = (np.arange(seq_len // PIECE) * PIECE)[:, None] * inv_freq
    off = np.arange(PIECE)[:, None] * inv_freq
    return [jnp.asarray(t, F32) for t in (np.cos(base), sign * np.sin(base), np.cos(off), sign * np.sin(off))]


def block_kernel(
    n, x_hbm, gain, wq_hbm, wk_hbm, wv_hbm, wo_hbm, q_gain, k_gain, cos_b, sin_b, cos_o, sin_o,
    out_hbm, k_hbm, v_hbm,
    hbuf, wqkv, wo, q_s, k_f, v_s, v_t, ybuf, o_s, kv_st, sq_out, sq_in, sums,
    ld_sem, ag_send, ag_recv, dd_send, dd_recv, sq_send, sq_recv, iv_send, iv_recv,
    rs_send, rs_recv, sb_send, sb_recv, st_sem, out_sem,
):
    nz = n // 2
    me = lax.axis_index("tp")
    z, c = me // 2, lax.rem(me, 2)
    sib = z * 2 + 1 - c
    n_rows, width = x_hbm.shape
    half = n_rows // 2
    pieces = half // PIECE
    units = nz * pieces
    cols = q_s.shape[1]
    heads = cols // HEAD_DIM
    sub = half // SUM_PIECES
    k_tile = 2 * n_rows
    shares = units // 2
    cast_rows = q_s.shape[0] // (nz * SUM_PIECES)

    k_s = wqkv.at[0]

    def chip(offset):
        return lax.rem(z + offset + 2 * nz, nz)

    def toward(d, hops=1):
        return chip(hops) if d == 0 else chip(-hops)

    def rows(start, size):
        return pl.ds(pl.multiple_of(start, size), size)

    def remote(src, dst, send, recv, dev):
        return pltpu.make_async_remote_copy(
            src_ref=src, dst_ref=dst, send_sem=send, recv_sem=recv,
            device_id={"tp": dev}, device_id_type=pl.DeviceIdType.MESH)

    def wait_bytes(ref, sem):
        remote(ref, ref, sem, sem, sib).wait_recv()

    def x_load(d, p):
        at = pl.ds(d * half + p * PIECE, PIECE)
        return pltpu.make_async_copy(x_hbm.at[at], ybuf.at[0, d, pl.ds(p * PIECE, PIECE)], ld_sem.at[4 + d * pieces + p])

    for p in range(pieces):
        for d in range(2):
            x_load(d, p).start()
    loads = [pltpu.make_async_copy(w, wqkv.at[i, pl.ds(0, width)], ld_sem.at[i]) for i, w in enumerate((wq_hbm, wk_hbm, wv_hbm))]
    loads.append(pltpu.make_async_copy(wo_hbm, wo, ld_sem.at[3]))

    barrier = pltpu.get_barrier_semaphore()

    def greet(i, _):
        pl.semaphore_signal(barrier, inc=1, device_id={"tp": lax.rem(me + i, n)}, device_id_type=pl.DeviceIdType.MESH)
        return 0

    lax.fori_loop(1, n, greet, 0)

    def quarter(u, d):
        return hbuf.at[u, rows((2 * d + c) * PIECE, PIECE)]

    def ring_copy(u, d):
        return remote(quarter(u, d), quarter(u + pieces, d), ag_send.at[lax.rem(u, 4), d], ag_recv.at[u], toward(d) * 2 + c)

    def pair_copy(u, d):
        return remote(quarter(u, d), quarter(u, d), dd_send.at[lax.rem(u, 4), d], dd_recv.at[u], sib)

    for p in range(pieces):
        for d in range(2):
            x_load(d, p).wait()
            x = ybuf[0, d, pl.ds(p * PIECE, PIECE), :].astype(F32)
            inv_rms = lax.rsqrt(jnp.mean(x * x, axis=-1, keepdims=True) + EPS)
            hbuf[p, rows((2 * d + c) * PIECE, PIECE), :] = (x * inv_rms * gain[...]).astype(BF16)
        if p == 0:
            for load in loads:
                load.start()
            pl.semaphore_wait(barrier, n - 1)
        for d in range(2):
            ring_copy(p, d).start()
            pair_copy(p, d).start()

    def sq_copy(u, d, p, dev):
        return remote(sq_out.at[u, d], sq_in.at[z, d, p], sq_send.at[lax.rem(u, 4), d], sq_recv, dev)

    def rotate(t, src, d, cc, p):
        b = (2 * src + cc) * (n_rows // PIECE) + d * pieces + p
        cb, sb = cos_b[pl.ds(b, 1), :], sin_b[pl.ds(b, 1), :]
        cos = cb * cos_o[...] - sb * sin_o[...]
        sin = sb * cos_o[...] + cb * sin_o[...]
        heads_in = [t[:, j * HEAD_DIM:(j + 1) * HEAD_DIM] for j in range(heads)]
        return [x * cos + pltpu.roll(x, HEAD_DIM // 2, 1) * sin for x in heads_in]

    def project(v):
        s, p = v // pieces, lax.rem(v, pieces)
        wait_bytes(hbuf.at[v, pl.ds(0, 2 * PIECE)], dd_recv.at[v])

        @pl.when(v == 0)
        def _():
            for load in loads:
                load.wait()

        h = hbuf[v]
        parts = [(d, cc, chip(-s) if d == 0 else chip(s), (2 * d + cc) * PIECE) for d in range(2) for cc in range(2)]

        def at(d, cc, src):
            return rows((2 * src + cc) * n_rows + d * half + p * PIECE, PIECE)

        outs, squares = [], []
        for i in range(2):
            out = jnp.dot(h, wqkv[i, :width], preferred_element_type=F32).astype(BF16)
            wide = out.astype(F32)
            sq = wide * wide
            lanes = sq[:, :HEAD_DIM]
            for j in range(1, heads):
                lanes = lanes + sq[:, j * HEAD_DIM:(j + 1) * HEAD_DIM]
            outs.append(out)
            squares.append(lanes)
        for d, cc, src, lo in parts:
            q_s[at(d, cc, src), :] = outs[0][lo:lo + PIECE]
            k_f[at(d, cc, src), :] = outs[1][lo:lo + PIECE].astype(F32)
        for d in range(2):
            for i in range(2):
                part = squares[i][d * 2 * PIECE:(d + 1) * 2 * PIECE]
                sq_out[v, d, pl.ds(i, 1), :] = jnp.sum(part.T, axis=0, keepdims=True)
            owner = chip(-s - 1) if d == 0 else chip(s + 1)

            @pl.when(s < nz - 1)
            def _(d=d, owner=owner):
                sq_copy(v, d, p, owner * 2 + c).start()

            @pl.when(s == nz - 1)
            def _(d=d):
                sq_in[z, d, p] = sq_out[v, d]

    def project_rest(v):
        s, p = v // pieces, lax.rem(v, pieces)
        out = jnp.dot(hbuf[v], wqkv[2, :width], preferred_element_type=F32).astype(BF16)
        for d in range(2):
            src = chip(-s) if d == 0 else chip(s)
            for cc in range(2):
                at = rows((2 * src + cc) * n_rows + d * half + p * PIECE, PIECE)
                lo = (2 * d + cc) * PIECE
                v_s[at, :] = out[lo:lo + PIECE]
                done = rotate(k_f[at, :] * k_gain[...], src, d, cc, p)
                for j in range(heads):
                    k_f[at, j * HEAD_DIM:(j + 1) * HEAD_DIM] = done[j]

    def drain(u):
        for d in range(2):
            pair_copy(u, d).wait_send()

            @pl.when(u < units - pieces)
            def _(d=d):
                ring_copy(u, d).wait_send()
                sq_copy(u, d, 0, sib).wait_send()

    def gather_step(u, _):
        @pl.when(u >= pieces)
        def _():
            wait_bytes(hbuf.at[u, pl.ds(0, 2 * PIECE)], ag_recv.at[u - pieces])
            for d in range(2):
                @pl.when(u < units - pieces)
                def _(d=d):
                    ring_copy(u, d).start()

                pair_copy(u, d).start()

        project(u)

        @pl.when(u >= 2)
        def _():
            drain(u - 2)

        @pl.when(u < units - 1)
        def _():
            project_rest(u)

        return 0

    lax.fori_loop(0, units, gather_step, 0)
    drain(units - 2)
    drain(units - 1)

    wait_bytes(sq_in.at[pl.ds(0, nz - 1)], sq_recv)
    total = sq_in[0]
    for i in range(1, nz):
        total = total + sq_in[i]
    sums[me] = total

    def inv_copy(i):
        dev = lax.rem(me + i, n)
        return remote(sums.at[me], sums.at[me], iv_send, iv_recv, dev)

    def inv_start(i, _):
        inv_copy(i).start()
        return 0

    lax.fori_loop(1, n, inv_start, 0)
    project_rest(units - 1)

    def turn_values(i, _):
        at = rows(i * k_tile, k_tile)
        v_t[:, at] = v_s[at, :].T
        return 0

    lax.fori_loop(0, q_s.shape[0] // k_tile, turn_values, 0)
    others = sums.at[pl.ds(0, n - 1)]
    wait_bytes(others, iv_recv)
    remote(others, others, iv_send, iv_recv, sib).wait_send()

    def row_scale(which, src, d, p):
        own = lax.rem(src + (nz - 1 if d == 0 else 1), nz) * 2
        total = sums[own, d, p][which:which + 1] + sums[own + 1, d, p][which:which + 1]
        return jnp.broadcast_to(lax.rsqrt(total / (cols * n) + EPS), (HEAD_DIM, HEAD_DIM)).T

    def piece_rows(src, cc, d, p):
        return rows((2 * src + cc) * n_rows + d * half + p * PIECE, PIECE)

    def finish_keys(src, _):
        for d in range(2):
            for p in range(pieces):
                scale = row_scale(1, src, d, p)
                for cc in range(2):
                    at = piece_rows(src, cc, d, p)
                    for j in range(heads):
                        lanes = slice(j * HEAD_DIM, (j + 1) * HEAD_DIM)
                        k_s[at, lanes] = (k_f[at, lanes] * scale[cc * PIECE:(cc + 1) * PIECE]).astype(BF16)
        return 0

    lax.fori_loop(0, nz, finish_keys, 0)

    scale = HEAD_DIM ** -0.5 * math.log2(math.e)

    queries = 2 * PIECE

    def attend(t, d, p):
        blk = lax.rem(z + 2 * nz - 1 - t, nz) if d == 0 else lax.rem(z + 1 + t, nz)
        factor = row_scale(0, blk, d, p)
        factor = jnp.concatenate([factor] * heads, axis=1)
        parts = []
        for cc in range(2):
            raw = q_s[piece_rows(blk, cc, d, p), :].astype(F32)
            parts.append(rotate(raw * factor[cc * PIECE:(cc + 1) * PIECE] * q_gain[...], blk, d, cc, p))
        q_t = [jnp.concatenate([parts[0][j], parts[1][j]], axis=0).T.astype(BF16) for j in range(heads)]

        def tile(at, carry, mask):
            lanes = [slice(j * HEAD_DIM, (j + 1) * HEAD_DIM) for j in range(heads)]
            score = [jnp.dot(k_s[at, lanes[j]], q_t[j], preferred_element_type=F32) for j in range(heads)]
            if mask is not None:
                score = [jnp.where(mask, sc, -1e30) for sc in score]
            peak = [jnp.maximum(carry[j][0], jnp.max(score[j], axis=0, keepdims=True)) for j in range(heads)]
            prob = [jnp.exp2(score[j] * scale - peak[j] * scale) for j in range(heads)]
            fade = [jnp.exp2((carry[j][0] - peak[j]) * scale) for j in range(heads)]
            acc = [jnp.dot(v_t[lanes[j], at], prob[j].astype(BF16), preferred_element_type=F32) for j in range(heads)]
            return tuple(
                (peak[j], carry[j][1] * fade[j] + jnp.sum(prob[j], axis=0, keepdims=True), carry[j][2] * fade[j] + acc[j])
                for j in range(heads))

        zero = (jnp.full((1, queries), -1e30, F32), jnp.zeros((1, queries), F32), jnp.zeros((HEAD_DIM, queries), F32))
        carry = lax.fori_loop(0, blk, lambda i, kept: tile(rows(i * k_tile, k_tile), kept, None), (zero,) * heads)
        key = lax.broadcasted_iota(jnp.int32, (k_tile, queries), 0)
        r = lax.broadcasted_iota(jnp.int32, (k_tile, queries), 1)
        mask = jnp.where(r < PIECE, r, r + (n_rows - PIECE)) + (d * half + p * PIECE) >= key
        carry = tile(rows(blk * k_tile, k_tile), carry, mask)
        for j in range(heads):
            _, l, acc = carry[j]
            o_s[:, j * HEAD_DIM:(j + 1) * HEAD_DIM] = (acc / l).T.astype(BF16)

    def share_copy(t, d, p):
        return remote(
            ybuf.at[1, d, pl.ds(p * PIECE, PIECE)], hbuf.at[shares + t, pl.ds(d * half + p * PIECE, PIECE)],
            sb_send.at[d * pieces + p], sb_recv.at[t, p], sib)

    y_tile, e_tile = min(width, 1024), min(width, 2048)

    def emit(t, d, p):
        @pl.when(t >= 1)
        def _():
            share_copy(t - 1, d, p).wait_send()

        def column(i, _):
            at = rows(i * e_tile, e_tile)
            y = jnp.dot(o_s[...], wo[:, at], preferred_element_type=F32).astype(BF16)
            for cc in range(2):
                ybuf[cc + c - 2 * cc * c, d, pl.ds(p * PIECE, PIECE), at] = y[cc * PIECE:(cc + 1) * PIECE]
            return 0

        lax.fori_loop(0, width // e_tile, column, 0)
        share_copy(t, d, p).start()

    def sum_copy(s, d, k):
        at = rows(d * half + k * sub, sub)
        return remote(hbuf.at[s, at], hbuf.at[s + 1, at], rs_send.at[d * SUM_PIECES + k],
                      rs_recv.at[s, k], toward(d) * 2 + c)

    def out_copy(d, k):
        at = rows(d * half + k * sub, sub)
        return pltpu.make_async_copy(hbuf.at[nz - 1, at], out_hbm.at[at], out_sem.at[d * SUM_PIECES + k])

    def add_up(s, k):
        if k * sub % PIECE == 0:
            wait_bytes(hbuf.at[shares + s, pl.ds(0, 2 * PIECE)], sb_recv.at[s, k * sub // PIECE])

        @pl.when(s >= 1)
        def _():
            wait_bytes(hbuf.at[s, pl.ds(0, 2 * sub)], rs_recv.at[s - 1, k])

        for d in range(2):
            at = rows(d * half + k * sub, sub)

            def column(i, _, d=d, at=at):
                lanes = rows(i * y_tile, y_tile)
                y = ybuf[0, d, pl.ds(k * sub, sub), lanes].astype(F32)
                y = y + hbuf[shares + s, at, lanes].astype(F32)
                run = hbuf[s, at, lanes].astype(F32)
                y = (y + jnp.where(s >= 1, run, 0.0)).astype(BF16)
                hbuf[s, at, lanes] = y

                @pl.when(s == nz - 1)
                def _():
                    hbuf[s, at, lanes] = (hbuf[shares, at, lanes].astype(F32) + y.astype(F32)).astype(BF16)

                return 0

            lax.fori_loop(0, width // y_tile, column, 0)

            @pl.when(s >= 1)
            def _(d=d):
                sum_copy(s - 1, d, k).wait_send()

            @pl.when(s < nz - 1)
            def _(d=d):
                sum_copy(s, d, k).start()

            @pl.when(s == nz - 1)
            def _(d=d):
                out_copy(d, k).start()

    x_again = pltpu.make_async_copy(x_hbm, hbuf.at[shares], ld_sem.at[0])

    def cache_copy(i, which):
        at = rows(i * cast_rows, cast_rows)
        return pltpu.make_async_copy(
            kv_st.at[which, lax.rem(i, 2)], (k_hbm, v_hbm)[which].at[at], st_sem.at[which, lax.rem(i, 2)])

    def write_caches(i):
        for which in range(2):
            @pl.when(i >= 2)
            def _(which=which):
                cache_copy(i - 2, which).wait()

            part = (k_s, v_s)[which][rows(i * cast_rows, cast_rows), :]
            kv_st[which, lax.rem(i, 2)] = part.reshape(cast_rows, heads, HEAD_DIM)
            cache_copy(i, which).start()

    def scatter_step(t, _):
        @pl.when(t == 2)
        def _():
            x_again.start()

        @pl.when(t == nz)
        def _():
            x_again.wait()

        for k in range(SUM_PIECES):
            @pl.when(t >= 1)
            def _(k=k):
                write_caches((t - 1) * SUM_PIECES + k)
                add_up(t - 1, k)

            d, late = k % 2, k < 2

            @pl.when((t >= 1) if late else (t < nz))
            def _(d=d, late=late):
                attend(t - late, d, int(late))
                emit(t - late, d, int(late))

        return 0

    lax.fori_loop(0, nz + 1, scatter_step, 0)

    for d in range(2):
        for p in range(pieces):
            share_copy(nz - 1, d, p).wait_send()
        for k in range(SUM_PIECES):
            out_copy(d, k).wait()
    for i in (nz * SUM_PIECES - 2, nz * SUM_PIECES - 1):
        for which in range(2):
            cache_copy(i, which).wait()


def flush_kernel(out_ref, k_ref, v_ref, out_hbm, k_hbm, v_hbm, sem):
    copies = []
    for i, (src, dst) in enumerate(((out_ref, out_hbm), (k_ref, k_hbm), (v_ref, v_hbm))):
        part = src.shape[0] // FLUSH_PARTS
        for j in range(FLUSH_PARTS):
            at = pl.ds(j * part, part)
            copies.append(pltpu.make_async_copy(src.at[at], dst.at[at], sem.at[i, j]))
    for copy in copies:
        copy.start()
    for copy in copies:
        copy.wait()


def solution(mesh):
    n = mesh.shape["tp"]

    def local_block(x_local, attn_gain, wq, wk, wv, q_gain, k_gain, wo):
        _, n_rows, width = x_local.shape
        cols = wq.shape[1]
        seq_len = n * n_rows
        nz, pieces = n // 2, n_rows // 2 // PIECE
        units = nz * pieces
        tables = rope_constants(seq_len)
        shapes = ((n_rows, width),) + ((seq_len, cols // HEAD_DIM, HEAD_DIM),) * 2
        any_spec = pl.BlockSpec(memory_space=pl.ANY)
        vmem_spec = pl.BlockSpec(memory_space=pltpu.VMEM)
        dma = pltpu.SemaphoreType.DMA
        held = pl.pallas_call(
            functools.partial(block_kernel, n),
            out_shape=tuple(pltpu.VMEM(shape, BF16) for shape in shapes),
            in_specs=[any_spec, vmem_spec] + [any_spec] * 4 + [vmem_spec] * 6,
            out_specs=(any_spec,) * 3,
            scratch_shapes=[
                pltpu.VMEM((units, 4 * PIECE, width), BF16),
                pltpu.VMEM((3, max(width, seq_len), cols), BF16),
                pltpu.VMEM((cols, width), BF16),
                pltpu.VMEM((seq_len, cols), BF16),
                pltpu.VMEM((seq_len, cols), F32),
                pltpu.VMEM((seq_len, cols), BF16),
                pltpu.VMEM((cols, seq_len), BF16),
                pltpu.VMEM((2, 2, n_rows // 2, width), BF16),
                pltpu.VMEM((2 * PIECE, cols), BF16),
                pltpu.VMEM((2, 2, seq_len // (nz * SUM_PIECES), cols // HEAD_DIM, HEAD_DIM), BF16),
                pltpu.VMEM((units, 2, 2, 2 * PIECE), F32),
                pltpu.VMEM((nz, 2, pieces, 2, 2 * PIECE), F32),
                pltpu.VMEM((n, 2, pieces, 2, 2 * PIECE), F32),
                dma((4 + 2 * pieces,)),
                dma((4, 2)), dma((units,)), dma((4, 2)), dma((units,)),
                dma((4, 2)), dma, dma, dma,
                dma((2 * SUM_PIECES,)), dma((nz - 1, SUM_PIECES)),
                dma((2 * pieces,)), dma((nz, pieces)), dma((2, 2)), dma((2 * SUM_PIECES,)),
            ],
            compiler_params=pltpu.CompilerParams(
                collective_id=0, has_side_effects=True, vmem_limit_bytes=KERNEL_VMEM),
            name="attention_block",
        )(x_local[0], attn_gain[None], wq, wk, wv, wo, q_gain[None], k_gain[None], *tables)
        out, k_rot, v_rows = pl.pallas_call(
            flush_kernel,
            out_shape=tuple(jax.ShapeDtypeStruct(shape, BF16) for shape in shapes),
            in_specs=[any_spec] * 3, out_specs=(any_spec,) * 3,
            scratch_shapes=[dma((3, FLUSH_PARTS))],
            compiler_params=pltpu.CompilerParams(vmem_limit_bytes=1 << 18),
            name="write_out",
        )(*held)
        return out[None], k_rot[None], v_rows[None]

    seq_spec = P("dp", "tp", None)
    head_spec = P("dp", None, "tp", None)
    col_spec = P(None, "tp")
    return jax.shard_map(
        local_block, mesh=mesh,
        in_specs=(seq_spec, P(None), col_spec, col_spec, col_spec, P("tp"), P("tp"), P("tp", None)),
        out_specs=(seq_spec, head_spec, head_spec), check_vma=False)
```

```python
import functools
import math

import jax
import jax.numpy as jnp
import numpy as np
from jax import lax
from jax.experimental import pallas as pl
from jax.experimental.pallas import tpu as pltpu
from jax.sharding import PartitionSpec as P

HEAD_DIM = 128
EPS = 1e-5
PIECE = 64
SUM_PIECES = 4
KERNEL_VMEM = 60700000
FLUSH_PARTS = 4
F32 = jnp.float32
BF16 = jnp.bfloat16


def rope_constants(seq_len):
    half = HEAD_DIM // 2
    inv_freq = 10000.0 ** (-np.arange(half) * (2.0 / HEAD_DIM))
    inv_freq = np.concatenate([inv_freq, inv_freq])
    sign = np.concatenate([-np.ones(half), np.ones(half)])
    base = (np.arange(seq_len // PIECE) * PIECE)[:, None] * inv_freq
    off = np.arange(PIECE)[:, None] * inv_freq
    return [jnp.asarray(t, F32) for t in (np.cos(base), sign * np.sin(base), np.cos(off), sign * np.sin(off))]


def block_kernel(
    n, x_hbm, gain, wq_hbm, wk_hbm, wv_hbm, wo_hbm, q_gain, k_gain, cos_b, sin_b, cos_o, sin_o,
    out_hbm, k_hbm, v_hbm,
    hbuf, wqkv, wo, q_s, k_f, v_s, v_t, ybuf, o_s, kv_st, sq_out, sq_in, sums,
    ld_sem, ag_send, ag_recv, dd_send, dd_recv, sq_send, sq_recv, iv_send, iv_recv,
    rs_send, rs_recv, sb_send, sb_recv, st_sem, out_sem,
):
    nz = n // 2
    me = lax.axis_index("tp")
    z, c = me // 2, lax.rem(me, 2)
    sib = z * 2 + 1 - c
    n_rows, width = x_hbm.shape
    half = n_rows // 2
    pieces = half // PIECE
    units = nz * pieces
    cols = q_s.shape[1]
    heads = cols // HEAD_DIM
    sub = half // SUM_PIECES
    k_tile = 2 * n_rows
    shares = units // 2
    cast_rows = q_s.shape[0] // (nz * SUM_PIECES)

    k_s = wqkv.at[0]

    def chip(offset):
        return lax.rem(z + offset + 2 * nz, nz)

    def toward(d, hops=1):
        return chip(hops) if d == 0 else chip(-hops)

    def rows(start, size):
        return pl.ds(pl.multiple_of(start, size), size)

    def remote(src, dst, send, recv, dev):
        return pltpu.make_async_remote_copy(
            src_ref=src, dst_ref=dst, send_sem=send, recv_sem=recv,
            device_id={"tp": dev}, device_id_type=pl.DeviceIdType.MESH)

    def wait_bytes(ref, sem):
        remote(ref, ref, sem, sem, sib).wait_recv()

    def x_load(d, p):
        at = pl.ds(d * half + p * PIECE, PIECE)
        return pltpu.make_async_copy(x_hbm.at[at], ybuf.at[0, d, pl.ds(p * PIECE, PIECE)], ld_sem.at[4 + d * pieces + p])

    for p in range(pieces):
        for d in range(2):
            x_load(d, p).start()
    loads = [pltpu.make_async_copy(w, wqkv.at[i, pl.ds(0, width)], ld_sem.at[i]) for i, w in enumerate((wq_hbm, wk_hbm, wv_hbm))]
    loads.append(pltpu.make_async_copy(wo_hbm, wo, ld_sem.at[3]))

    barrier = pltpu.get_barrier_semaphore()

    for dev in (sib, toward(0) * 2 + c, toward(1) * 2 + c):
        pl.semaphore_signal(barrier, inc=1, device_id={"tp": dev}, device_id_type=pl.DeviceIdType.MESH)

    def quarter(u, d):
        return hbuf.at[u, rows((2 * d + c) * PIECE, PIECE)]

    def ring_copy(u, d):
        return remote(quarter(u, d), quarter(u + pieces, d), ag_send.at[lax.rem(u, 4), d], ag_recv.at[u], toward(d) * 2 + c)

    def pair_copy(u, d):
        return remote(quarter(u, d), quarter(u, d), dd_send.at[lax.rem(u, 4), d], dd_recv.at[u], sib)

    for p in range(pieces):
        for d in range(2):
            x_load(d, p).wait()
            x = ybuf[0, d, pl.ds(p * PIECE, PIECE), :].astype(F32)
            inv_rms = lax.rsqrt(jnp.mean(x * x, axis=-1, keepdims=True) + EPS)
            hbuf[p, rows((2 * d + c) * PIECE, PIECE), :] = (x * inv_rms * gain[...]).astype(BF16)
        if p == 0:
            for load in loads:
                load.start()
            pl.semaphore_wait(barrier, 3)
        for d in range(2):
            ring_copy(p, d).start()
            pair_copy(p, d).start()

    def sq_copy(u, d, p, dev):
        return remote(sq_out.at[u, d], sq_in.at[z, d, p], sq_send.at[lax.rem(u, 4), d], sq_recv, dev)

    def rotate(t, src, d, cc, p):
        b = (2 * src + cc) * (n_rows // PIECE) + d * pieces + p
        cb, sb = cos_b[pl.ds(b, 1), :], sin_b[pl.ds(b, 1), :]
        cos = cb * cos_o[...] - sb * sin_o[...]
        sin = sb * cos_o[...] + cb * sin_o[...]
        heads_in = [t[:, j * HEAD_DIM:(j + 1) * HEAD_DIM] for j in range(heads)]
        return [x * cos + pltpu.roll(x, HEAD_DIM // 2, 1) * sin for x in heads_in]

    def project(v):
        s, p = v // pieces, lax.rem(v, pieces)
        wait_bytes(hbuf.at[v, pl.ds(0, 2 * PIECE)], dd_recv.at[v])

        @pl.when(v == 0)
        def _():
            for load in loads:
                load.wait()

        h = hbuf[v]
        parts = [(d, cc, chip(-s) if d == 0 else chip(s), (2 * d + cc) * PIECE) for d in range(2) for cc in range(2)]

        def at(d, cc, src):
            return rows((2 * src + cc) * n_rows + d * half + p * PIECE, PIECE)

        outs, squares = [], []
        for i in range(2):
            out = jnp.dot(h, wqkv[i, :width], preferred_element_type=F32).astype(BF16)
            wide = out.astype(F32)
            sq = wide * wide
            lanes = sq[:, :HEAD_DIM]
            for j in range(1, heads):
                lanes = lanes + sq[:, j * HEAD_DIM:(j + 1) * HEAD_DIM]
            outs.append(out)
            squares.append(lanes)
        for d, cc, src, lo in parts:
            q_s[at(d, cc, src), :] = outs[0][lo:lo + PIECE]
            k_f[at(d, cc, src), :] = outs[1][lo:lo + PIECE].astype(F32)
        for d in range(2):
            for i in range(2):
                part = squares[i][d * 2 * PIECE:(d + 1) * 2 * PIECE]
                sq_out[v, d, pl.ds(i, 1), :] = jnp.sum(part.T, axis=0, keepdims=True)
            owner = chip(-s - 1) if d == 0 else chip(s + 1)

            @pl.when(s < nz - 1)
            def _(d=d, owner=owner):
                sq_copy(v, d, p, owner * 2 + c).start()

            @pl.when(s == nz - 1)
            def _(d=d):
                sq_in[z, d, p] = sq_out[v, d]

    def project_rest(v):
        s, p = v // pieces, lax.rem(v, pieces)
        out = jnp.dot(hbuf[v], wqkv[2, :width], preferred_element_type=F32).astype(BF16)
        for d in range(2):
            src = chip(-s) if d == 0 else chip(s)
            for cc in range(2):
                at = rows((2 * src + cc) * n_rows + d * half + p * PIECE, PIECE)
                lo = (2 * d + cc) * PIECE
                v_s[at, :] = out[lo:lo + PIECE]
                done = rotate(k_f[at, :] * k_gain[...], src, d, cc, p)
                for j in range(heads):
                    k_f[at, j * HEAD_DIM:(j + 1) * HEAD_DIM] = done[j]

    def drain(u):
        for d in range(2):
            pair_copy(u, d).wait_send()

            @pl.when(u < units - pieces)
            def _(d=d):
                ring_copy(u, d).wait_send()
                sq_copy(u, d, 0, sib).wait_send()

    def gather_step(u, _):
        @pl.when(u >= pieces)
        def _():
            wait_bytes(hbuf.at[u, pl.ds(0, 2 * PIECE)], ag_recv.at[u - pieces])
            for d in range(2):
                @pl.when(u < units - pieces)
                def _(d=d):
                    ring_copy(u, d).start()

                pair_copy(u, d).start()

        project(u)

        @pl.when(u >= 2)
        def _():
            drain(u - 2)

        @pl.when(u < units - 1)
        def _():
            project_rest(u)

        return 0

    lax.fori_loop(0, units, gather_step, 0)
    drain(units - 2)
    drain(units - 1)

    wait_bytes(sq_in.at[pl.ds(0, nz - 1)], sq_recv)
    total = sq_in[0]
    for i in range(1, nz):
        total = total + sq_in[i]
    sums[me] = total

    def inv_copy(i):
        dev = lax.rem(me + i, n)
        return remote(sums.at[me], sums.at[me], iv_send, iv_recv, dev)

    def inv_start(i, _):
        inv_copy(i).start()
        return 0

    lax.fori_loop(1, n, inv_start, 0)
    project_rest(units - 1)

    def turn_values(i, _):
        at = rows(i * k_tile, k_tile)
        v_t[:, at] = v_s[at, :].T
        return 0

    lax.fori_loop(0, q_s.shape[0] // k_tile, turn_values, 0)
    others = sums.at[pl.ds(0, n - 1)]
    wait_bytes(others, iv_recv)
    remote(others, others, iv_send, iv_recv, sib).wait_send()

    def row_scale(which, src, d, p):
        own = lax.rem(src + (nz - 1 if d == 0 else 1), nz) * 2
        total = sums[own, d, p][which:which + 1] + sums[own + 1, d, p][which:which + 1]
        return jnp.broadcast_to(lax.rsqrt(total / (cols * n) + EPS), (HEAD_DIM, HEAD_DIM)).T

    def piece_rows(src, cc, d, p):
        return rows((2 * src + cc) * n_rows + d * half + p * PIECE, PIECE)

    def finish_keys(src, _):
        for d in range(2):
            for p in range(pieces):
                scale = row_scale(1, src, d, p)
                for cc in range(2):
                    at = piece_rows(src, cc, d, p)
                    for j in range(heads):
                        lanes = slice(j * HEAD_DIM, (j + 1) * HEAD_DIM)
                        k_s[at, lanes] = (k_f[at, lanes] * scale[cc * PIECE:(cc + 1) * PIECE]).astype(BF16)
        return 0

    lax.fori_loop(0, nz, finish_keys, 0)

    scale = HEAD_DIM ** -0.5 * math.log2(math.e)

    queries = 2 * PIECE

    def attend(t, d, p):
        blk = lax.rem(z + 2 * nz - 1 - t, nz) if d == 0 else lax.rem(z + 1 + t, nz)
        factor = row_scale(0, blk, d, p)
        factor = jnp.concatenate([factor] * heads, axis=1)
        parts = []
        for cc in range(2):
            raw = q_s[piece_rows(blk, cc, d, p), :].astype(F32)
            parts.append(rotate(raw * factor[cc * PIECE:(cc + 1) * PIECE] * q_gain[...], blk, d, cc, p))
        q_t = [jnp.concatenate([parts[0][j], parts[1][j]], axis=0).T.astype(BF16) for j in range(heads)]

        head = [slice(j * HEAD_DIM, (j + 1) * HEAD_DIM) for j in range(heads)]

        def scores(at):
            return [jnp.dot(k_s[at, head[j]], q_t[j], preferred_element_type=F32) for j in range(heads)]

        def update(at, score, carry):
            peak = [jnp.maximum(carry[j][0], jnp.max(score[j], axis=0, keepdims=True)) for j in range(heads)]
            prob = [jnp.exp2(score[j] * scale - peak[j] * scale) for j in range(heads)]
            fade = [jnp.exp2((carry[j][0] - peak[j]) * scale) for j in range(heads)]
            acc = [jnp.dot(v_t[head[j], at], prob[j].astype(BF16), preferred_element_type=F32) for j in range(heads)]
            return tuple(
                (peak[j], carry[j][1] * fade[j] + jnp.sum(prob[j], axis=0, keepdims=True), carry[j][2] * fade[j] + acc[j])
                for j in range(heads))

        def one(i, carry):
            at = rows(i * k_tile, k_tile)
            return update(at, scores(at), carry)

        def two(i, carry):
            at = [rows((2 * i + m) * k_tile, k_tile) for m in range(2)]
            both = [scores(a) for a in at]
            return update(at[1], both[1], update(at[0], both[0], carry))

        zero = (jnp.full((1, queries), -1e30, F32), jnp.zeros((1, queries), F32), jnp.zeros((HEAD_DIM, queries), F32))
        pairs = blk // 2
        carry = lax.fori_loop(0, pairs, two, (zero,) * heads)
        carry = lax.fori_loop(2 * pairs, blk, one, carry)
        key = lax.broadcasted_iota(jnp.int32, (k_tile, queries), 0)
        r = lax.broadcasted_iota(jnp.int32, (k_tile, queries), 1)
        mask = jnp.where(r < PIECE, r, r + (n_rows - PIECE)) + (d * half + p * PIECE) >= key
        at = rows(blk * k_tile, k_tile)
        carry = update(at, [jnp.where(mask, sc, -1e30) for sc in scores(at)], carry)
        for j in range(heads):
            _, l, acc = carry[j]
            o_s[:, j * HEAD_DIM:(j + 1) * HEAD_DIM] = (acc / l).T.astype(BF16)

    def share_copy(t, d, p):
        return remote(
            ybuf.at[1, d, pl.ds(p * PIECE, PIECE)], hbuf.at[shares + t, pl.ds(d * half + p * PIECE, PIECE)],
            sb_send.at[d * pieces + p], sb_recv.at[t, p], sib)

    y_tile, e_tile = min(width, 1024), min(width, 2048)

    def emit(t, d, p):
        @pl.when(t >= 1)
        def _():
            share_copy(t - 1, d, p).wait_send()

        def column(i, _):
            at = rows(i * e_tile, e_tile)
            y = jnp.dot(o_s[...], wo[:, at], preferred_element_type=F32).astype(BF16)
            for cc in range(2):
                ybuf[cc + c - 2 * cc * c, d, pl.ds(p * PIECE, PIECE), at] = y[cc * PIECE:(cc + 1) * PIECE]
            return 0

        lax.fori_loop(0, width // e_tile, column, 0)
        share_copy(t, d, p).start()

    def sum_copy(s, d, k):
        at = rows(d * half + k * sub, sub)
        return remote(hbuf.at[s, at], hbuf.at[s + 1, at], rs_send.at[d * SUM_PIECES + k],
                      rs_recv.at[s, k], toward(d) * 2 + c)

    def out_copy(d, k):
        at = rows(d * half + k * sub, sub)
        return pltpu.make_async_copy(hbuf.at[nz - 1, at], out_hbm.at[at], out_sem.at[d * SUM_PIECES + k])

    def add_up(s, k):
        if k * sub % PIECE == 0:
            wait_bytes(hbuf.at[shares + s, pl.ds(0, 2 * PIECE)], sb_recv.at[s, k * sub // PIECE])

        @pl.when(s >= 1)
        def _():
            wait_bytes(hbuf.at[s, pl.ds(0, 2 * sub)], rs_recv.at[s - 1, k])

        for d in range(2):
            at = rows(d * half + k * sub, sub)

            def column(i, _, d=d, at=at):
                lanes = rows(i * y_tile, y_tile)
                y = ybuf[0, d, pl.ds(k * sub, sub), lanes].astype(F32)
                y = y + hbuf[shares + s, at, lanes].astype(F32)
                run = hbuf[s, at, lanes].astype(F32)
                y = (y + jnp.where(s >= 1, run, 0.0)).astype(BF16)
                hbuf[s, at, lanes] = y

                @pl.when(s == nz - 1)
                def _():
                    hbuf[s, at, lanes] = (hbuf[shares, at, lanes].astype(F32) + y.astype(F32)).astype(BF16)

                return 0

            lax.fori_loop(0, width // y_tile, column, 0)

            @pl.when(s >= 1)
            def _(d=d):
                sum_copy(s - 1, d, k).wait_send()

            @pl.when(s < nz - 1)
            def _(d=d):
                sum_copy(s, d, k).start()

            @pl.when(s == nz - 1)
            def _(d=d):
                out_copy(d, k).start()

    x_again = pltpu.make_async_copy(x_hbm, hbuf.at[shares], ld_sem.at[0])

    def cache_copy(i, which):
        at = rows(i * cast_rows, cast_rows)
        return pltpu.make_async_copy(
            kv_st.at[which, lax.rem(i, 2)], (k_hbm, v_hbm)[which].at[at], st_sem.at[which, lax.rem(i, 2)])

    def write_caches(i):
        for which in range(2):
            @pl.when(i >= 2)
            def _(which=which):
                cache_copy(i - 2, which).wait()

            part = (k_s, v_s)[which][rows(i * cast_rows, cast_rows), :]
            kv_st[which, lax.rem(i, 2)] = part.reshape(cast_rows, heads, HEAD_DIM)
            cache_copy(i, which).start()

    def scatter_step(t, _):
        @pl.when(t == 2)
        def _():
            x_again.start()

        @pl.when(t == nz)
        def _():
            x_again.wait()

        for k in range(SUM_PIECES):
            @pl.when(t >= 1)
            def _(k=k):
                write_caches((t - 1) * SUM_PIECES + k)
                add_up(t - 1, k)

            d, late = k % 2, k < 2

            @pl.when((t >= 1) if late else (t < nz))
            def _(d=d, late=late):
                attend(t - late, d, int(late))
                emit(t - late, d, int(late))

        return 0

    lax.fori_loop(0, nz + 1, scatter_step, 0)

    for d in range(2):
        for p in range(pieces):
            share_copy(nz - 1, d, p).wait_send()
        for k in range(SUM_PIECES):
            out_copy(d, k).wait()
    for i in (nz * SUM_PIECES - 2, nz * SUM_PIECES - 1):
        for which in range(2):
            cache_copy(i, which).wait()


def flush_kernel(out_ref, k_ref, v_ref, out_hbm, k_hbm, v_hbm, sem):
    copies = []
    for i, (src, dst) in enumerate(((out_ref, out_hbm), (k_ref, k_hbm), (v_ref, v_hbm))):
        part = src.shape[0] // FLUSH_PARTS
        for j in range(FLUSH_PARTS):
            at = pl.ds(j * part, part)
            copies.append(pltpu.make_async_copy(src.at[at], dst.at[at], sem.at[i, j]))
    for copy in copies:
        copy.start()
    for copy in copies:
        copy.wait()


def solution(mesh):
    n = mesh.shape["tp"]

    def local_block(x_local, attn_gain, wq, wk, wv, q_gain, k_gain, wo):
        _, n_rows, width = x_local.shape
        cols = wq.shape[1]
        seq_len = n * n_rows
        nz, pieces = n // 2, n_rows // 2 // PIECE
        units = nz * pieces
        tables = rope_constants(seq_len)
        shapes = ((n_rows, width),) + ((seq_len, cols // HEAD_DIM, HEAD_DIM),) * 2
        any_spec = pl.BlockSpec(memory_space=pl.ANY)
        vmem_spec = pl.BlockSpec(memory_space=pltpu.VMEM)
        dma = pltpu.SemaphoreType.DMA
        held = pl.pallas_call(
            functools.partial(block_kernel, n),
            out_shape=tuple(pltpu.VMEM(shape, BF16) for shape in shapes),
            in_specs=[any_spec, vmem_spec] + [any_spec] * 4 + [vmem_spec] * 6,
            out_specs=(any_spec,) * 3,
            scratch_shapes=[
                pltpu.VMEM((units, 4 * PIECE, width), BF16),
                pltpu.VMEM((3, max(width, seq_len), cols), BF16),
                pltpu.VMEM((cols, width), BF16),
                pltpu.VMEM((seq_len, cols), BF16),
                pltpu.VMEM((seq_len, cols), F32),
                pltpu.VMEM((seq_len, cols), BF16),
                pltpu.VMEM((cols, seq_len), BF16),
                pltpu.VMEM((2, 2, n_rows // 2, width), BF16),
                pltpu.VMEM((2 * PIECE, cols), BF16),
                pltpu.VMEM((2, 2, seq_len // (nz * SUM_PIECES), cols // HEAD_DIM, HEAD_DIM), BF16),
                pltpu.VMEM((units, 2, 2, 2 * PIECE), F32),
                pltpu.VMEM((nz, 2, pieces, 2, 2 * PIECE), F32),
                pltpu.VMEM((n, 2, pieces, 2, 2 * PIECE), F32),
                dma((4 + 2 * pieces,)),
                dma((4, 2)), dma((units,)), dma((4, 2)), dma((units,)),
                dma((4, 2)), dma, dma, dma,
                dma((2 * SUM_PIECES,)), dma((nz - 1, SUM_PIECES)),
                dma((2 * pieces,)), dma((nz, pieces)), dma((2, 2)), dma((2 * SUM_PIECES,)),
            ],
            compiler_params=pltpu.CompilerParams(
                collective_id=0, has_side_effects=True, vmem_limit_bytes=KERNEL_VMEM),
            name="attention_block",
        )(x_local[0], attn_gain[None], wq, wk, wv, wo, q_gain[None], k_gain[None], *tables)
        out, k_rot, v_rows = pl.pallas_call(
            flush_kernel,
            out_shape=tuple(jax.ShapeDtypeStruct(shape, BF16) for shape in shapes),
            in_specs=[any_spec] * 3, out_specs=(any_spec,) * 3,
            scratch_shapes=[dma((3, FLUSH_PARTS))],
            compiler_params=pltpu.CompilerParams(vmem_limit_bytes=1 << 18),
            name="write_out",
        )(*held)
        return out[None], k_rot[None], v_rows[None]

    seq_spec = P("dp", "tp", None)
    head_spec = P("dp", None, "tp", None)
    col_spec = P(None, "tp")
    return jax.shard_map(
        local_block, mesh=mesh,
        in_specs=(seq_spec, P(None), col_spec, col_spec, col_spec, P("tp"), P("tp"), P("tp", None)),
        out_specs=(seq_spec, head_spec, head_spec), check_vma=False)
```

```python
import functools
import math

import jax
import jax.numpy as jnp
import numpy as np
from jax import lax
from jax.experimental import pallas as pl
from jax.experimental.pallas import tpu as pltpu
from jax.sharding import PartitionSpec as P

HEAD_DIM = 128
EPS = 1e-5
PIECE = 64
SUM_PIECES = 4
KERNEL_VMEM = 60700000
FLUSH_PARTS = 4
F32 = jnp.float32
BF16 = jnp.bfloat16


def rope_constants(seq_len):
    half = HEAD_DIM // 2
    inv_freq = 10000.0 ** (-np.arange(half) * (2.0 / HEAD_DIM))
    inv_freq = np.concatenate([inv_freq, inv_freq])
    sign = np.concatenate([-np.ones(half), np.ones(half)])
    base = (np.arange(seq_len // PIECE) * PIECE)[:, None] * inv_freq
    off = np.arange(PIECE)[:, None] * inv_freq
    return [jnp.asarray(t, F32) for t in (np.cos(base), sign * np.sin(base), np.cos(off), sign * np.sin(off))]


def block_kernel(
    n, x_hbm, gain, wq_hbm, wk_hbm, wv_hbm, wo_hbm, q_gain, k_gain, cos_b, sin_b, cos_o, sin_o,
    out_hbm, k_hbm, v_hbm,
    hbuf, wqkv, wo, q_s, k_f, v_s, v_t, ybuf, o_s, kv_st, sq_out, sq_in, sums,
    ld_sem, ag_send, ag_recv, dd_send, dd_recv, sq_send, sq_recv, iv_send, iv_recv,
    rs_send, rs_recv, sb_send, sb_recv, st_sem, out_sem,
):
    nz = n // 2
    me = lax.axis_index("tp")
    z, c = me // 2, lax.rem(me, 2)
    sib = z * 2 + 1 - c
    n_rows, width = x_hbm.shape
    half = n_rows // 2
    pieces = half // PIECE
    units = nz * pieces
    cols = q_s.shape[1]
    heads = cols // HEAD_DIM
    sub = half // SUM_PIECES
    k_tile = 2 * n_rows
    shares = units // 2
    cast_rows = q_s.shape[0] // (nz * SUM_PIECES)

    k_s = wqkv.at[0]

    def chip(offset):
        return lax.rem(z + offset + 2 * nz, nz)

    def toward(d, hops=1):
        return chip(hops) if d == 0 else chip(-hops)

    def rows(start, size):
        return pl.ds(pl.multiple_of(start, size), size)

    def remote(src, dst, send, recv, dev):
        return pltpu.make_async_remote_copy(
            src_ref=src, dst_ref=dst, send_sem=send, recv_sem=recv,
            device_id={"tp": dev}, device_id_type=pl.DeviceIdType.MESH)

    def wait_bytes(ref, sem):
        remote(ref, ref, sem, sem, sib).wait_recv()

    def x_load(d, p):
        at = pl.ds(d * half + p * PIECE, PIECE)
        return pltpu.make_async_copy(x_hbm.at[at], ybuf.at[0, d, pl.ds(p * PIECE, PIECE)], ld_sem.at[4 + d * pieces + p])

    for p in range(pieces):
        for d in range(2):
            x_load(d, p).start()
    loads = [pltpu.make_async_copy(w, wqkv.at[i, pl.ds(0, width)], ld_sem.at[i]) for i, w in enumerate((wq_hbm, wk_hbm, wv_hbm))]
    loads.append(pltpu.make_async_copy(wo_hbm, wo, ld_sem.at[3]))

    barrier = pltpu.get_barrier_semaphore()

    for dev in (sib, toward(0) * 2 + c, toward(1) * 2 + c):
        pl.semaphore_signal(barrier, inc=1, device_id={"tp": dev}, device_id_type=pl.DeviceIdType.MESH)

    def quarter(u, d):
        return hbuf.at[u, rows((2 * d + c) * PIECE, PIECE)]

    def ring_copy(u, d):
        return remote(quarter(u, d), quarter(u + pieces, d), ag_send.at[lax.rem(u, 4)], ag_recv.at[u], toward(d) * 2 + c)

    def pair_copy(u, d):
        return remote(quarter(u, d), quarter(u, d), dd_send.at[lax.rem(u, 4)], dd_recv.at[u], sib)

    for p in range(pieces):
        for d in range(2):
            x_load(d, p).wait()
            x = ybuf[0, d, pl.ds(p * PIECE, PIECE), :].astype(F32)
            inv_rms = lax.rsqrt(jnp.mean(x * x, axis=-1, keepdims=True) + EPS)
            hbuf[p, rows((2 * d + c) * PIECE, PIECE), :] = (x * inv_rms * gain[...]).astype(BF16)
        if p == 0:
            for load in loads:
                load.start()
            pl.semaphore_wait(barrier, 3)
        for d in range(2):
            ring_copy(p, d).start()
            pair_copy(p, d).start()

    def sq_copy(u, d, p, dev):
        return remote(sq_out.at[u, d], sq_in.at[z, d, p], sq_send.at[lax.rem(u, 4)], sq_recv, dev)

    def rotate(t, src, d, cc, p):
        b = (2 * src + cc) * (n_rows // PIECE) + d * pieces + p
        cb, sb = cos_b[pl.ds(b, 1), :], sin_b[pl.ds(b, 1), :]
        cos = cb * cos_o[...] - sb * sin_o[...]
        sin = sb * cos_o[...] + cb * sin_o[...]
        heads_in = [t[:, j * HEAD_DIM:(j + 1) * HEAD_DIM] for j in range(heads)]
        return [x * cos + pltpu.roll(x, HEAD_DIM // 2, 1) * sin for x in heads_in]

    def project(v):
        s, p = v // pieces, lax.rem(v, pieces)
        wait_bytes(hbuf.at[v, pl.ds(0, 2 * PIECE)], dd_recv.at[v])

        @pl.when(v == 0)
        def _():
            for load in loads:
                load.wait()

        h = hbuf[v]
        parts = [(d, cc, chip(-s) if d == 0 else chip(s), (2 * d + cc) * PIECE) for d in range(2) for cc in range(2)]

        def at(d, cc, src):
            return rows((2 * src + cc) * n_rows + d * half + p * PIECE, PIECE)

        outs, squares = [], []
        for i in range(2):
            out = jnp.dot(h, wqkv[i, :width], preferred_element_type=F32).astype(BF16)
            wide = out.astype(F32)
            sq = wide * wide
            lanes = sq[:, :HEAD_DIM]
            for j in range(1, heads):
                lanes = lanes + sq[:, j * HEAD_DIM:(j + 1) * HEAD_DIM]
            outs.append(out)
            squares.append(lanes)
        for d in range(2):
            for i in range(2):
                part = squares[i][d * 2 * PIECE:(d + 1) * 2 * PIECE]
                sq_out[v, d, pl.ds(i, 1), :] = jnp.sum(part.T, axis=0, keepdims=True)
            owner = chip(-s - 1) if d == 0 else chip(s + 1)

            @pl.when(s < nz - 1)
            def _(d=d, owner=owner):
                sq_copy(v, d, p, owner * 2 + c).start()

            @pl.when(s == nz - 1)
            def _(d=d):
                sq_in[z, d, p] = sq_out[v, d]

        for d, cc, src, lo in parts:
            q_s[at(d, cc, src), :] = outs[0][lo:lo + PIECE]
            k_f[at(d, cc, src), :] = outs[1][lo:lo + PIECE].astype(F32)

    def project_rest(v):
        s, p = v // pieces, lax.rem(v, pieces)
        out = jnp.dot(hbuf[v], wqkv[2, :width], preferred_element_type=F32).astype(BF16)
        for d in range(2):
            src = chip(-s) if d == 0 else chip(s)
            for cc in range(2):
                at = rows((2 * src + cc) * n_rows + d * half + p * PIECE, PIECE)
                lo = (2 * d + cc) * PIECE
                v_s[at, :] = out[lo:lo + PIECE]
                done = rotate(k_f[at, :] * k_gain[...], src, d, cc, p)
                for j in range(heads):
                    k_f[at, j * HEAD_DIM:(j + 1) * HEAD_DIM] = done[j]

    def sent_bytes(ref, sem):
        remote(ref, ref, sem, sem, sib).wait_send()

    def drain(u):
        both = hbuf.at[u, pl.ds(0, 2 * PIECE)]
        sent_bytes(both, dd_send.at[lax.rem(u, 4)])

        @pl.when(u < units - pieces)
        def _():
            sent_bytes(both, ag_send.at[lax.rem(u, 4)])
            sent_bytes(sq_out.at[u], sq_send.at[lax.rem(u, 4)])

    def gather_step(u, _):
        @pl.when(u >= pieces)
        def _():
            wait_bytes(hbuf.at[u, pl.ds(0, 2 * PIECE)], ag_recv.at[u - pieces])
            for d in range(2):
                @pl.when(u < units - pieces)
                def _(d=d):
                    ring_copy(u, d).start()

                pair_copy(u, d).start()

        project(u)

        @pl.when(u >= 2)
        def _():
            drain(u - 2)

        @pl.when(u < units - 1)
        def _():
            project_rest(u)

        return 0

    lax.fori_loop(0, units, gather_step, 0)
    drain(units - 2)
    drain(units - 1)

    wait_bytes(sq_in.at[pl.ds(0, nz - 1)], sq_recv)
    total = sq_in[0]
    for i in range(1, nz):
        total = total + sq_in[i]
    sums[me] = total

    def inv_start(i, _):
        dev = lax.rem(me + n // 2 + i // 2 * (1 - 2 * lax.rem(i, 2)) + n, n)
        remote(sums.at[me], sums.at[me], iv_send, iv_recv.at[z], dev).start()
        return 0

    def sums_of(offset):
        at = sums.at[pl.ds(0, 1 if offset == 0 else 2)]
        wait_bytes(at, iv_recv.at[chip(offset)])

    lax.fori_loop(1, n, inv_start, 0)
    project_rest(units - 1)

    def turn_values(i, _):
        at = rows(i * k_tile, k_tile)
        v_t[:, at] = v_s[at, :].T
        return 0

    lax.fori_loop(0, q_s.shape[0] // k_tile, turn_values, 0)
    def row_scale(which, src, d, p):
        own = lax.rem(src + (nz - 1 if d == 0 else 1), nz) * 2
        total = sums[own, d, p][which:which + 1] + sums[own + 1, d, p][which:which + 1]
        return jnp.broadcast_to(lax.rsqrt(total / (cols * n) + EPS), (HEAD_DIM, HEAD_DIM)).T

    def piece_rows(src, cc, d, p):
        return rows((2 * src + cc) * n_rows + d * half + p * PIECE, PIECE)

    def finish_keys(src):
        for d in range(2):
            for p in range(pieces):
                scale = row_scale(1, src, d, p)
                for cc in range(2):
                    at = piece_rows(src, cc, d, p)
                    for j in range(heads):
                        lanes = slice(j * HEAD_DIM, (j + 1) * HEAD_DIM)
                        k_s[at, lanes] = (k_f[at, lanes] * scale[cc * PIECE:(cc + 1) * PIECE]).astype(BF16)

    def finish_near(distance):
        for offset in sorted({distance, -distance % nz}):
            finish_keys(chip(offset))

    sums_of(0)
    for distance in range(1, nz // 2 + 1):
        for offset in sorted({distance, -distance % nz}):
            sums_of(offset)
        finish_near(distance - 1)
        if distance == nz // 2 - 1:
            finish_near(nz // 2)
    others = sums.at[pl.ds(0, n - 1)]
    sent_bytes(others, iv_send)

    scale = HEAD_DIM ** -0.5 * math.log2(math.e)

    queries = 2 * PIECE

    def attend(t, d, p):
        blk = lax.rem(z + 2 * nz - 1 - t, nz) if d == 0 else lax.rem(z + 1 + t, nz)
        factor = row_scale(0, blk, d, p)
        factor = jnp.concatenate([factor] * heads, axis=1)
        parts = []
        for cc in range(2):
            raw = q_s[piece_rows(blk, cc, d, p), :].astype(F32)
            parts.append(rotate(raw * factor[cc * PIECE:(cc + 1) * PIECE] * q_gain[...], blk, d, cc, p))
        q_t = [jnp.concatenate([parts[0][j], parts[1][j]], axis=0).T.astype(BF16) for j in range(heads)]

        head = [slice(j * HEAD_DIM, (j + 1) * HEAD_DIM) for j in range(heads)]

        def scores(at):
            return [jnp.dot(k_s[at, head[j]], q_t[j], preferred_element_type=F32) for j in range(heads)]

        def update(at, score, carry):
            peak = [jnp.maximum(carry[j][0], jnp.max(score[j], axis=0, keepdims=True)) for j in range(heads)]
            prob = [jnp.exp2(score[j] * scale - peak[j] * scale) for j in range(heads)]
            fade = [jnp.exp2((carry[j][0] - peak[j]) * scale) for j in range(heads)]
            acc = [jnp.dot(v_t[head[j], at], prob[j].astype(BF16), preferred_element_type=F32) for j in range(heads)]
            return tuple(
                (peak[j], carry[j][1] * fade[j] + jnp.sum(prob[j], axis=0, keepdims=True), carry[j][2] * fade[j] + acc[j])
                for j in range(heads))

        def one(i, carry):
            at = rows(i * k_tile, k_tile)
            return update(at, scores(at), carry)

        def two(i, carry):
            at = [rows((2 * i + m) * k_tile, k_tile) for m in range(2)]
            both = [scores(a) for a in at]
            return update(at[1], both[1], update(at[0], both[0], carry))

        zero = (jnp.full((1, queries), -1e30, F32), jnp.zeros((1, queries), F32), jnp.zeros((HEAD_DIM, queries), F32))
        pairs = blk // 2
        carry = lax.fori_loop(0, pairs, two, (zero,) * heads)
        carry = lax.fori_loop(2 * pairs, blk, one, carry)
        key = lax.broadcasted_iota(jnp.int32, (k_tile, queries), 0)
        r = lax.broadcasted_iota(jnp.int32, (k_tile, queries), 1)
        mask = jnp.where(r < PIECE, r, r + (n_rows - PIECE)) + (d * half + p * PIECE) >= key
        at = rows(blk * k_tile, k_tile)
        carry = update(at, [jnp.where(mask, sc, -1e30) for sc in scores(at)], carry)
        for j in range(heads):
            _, l, acc = carry[j]
            o_s[:, j * HEAD_DIM:(j + 1) * HEAD_DIM] = (acc / l).T.astype(BF16)

    y_tile, e_tile = min(width, 1024), min(width, 2048)

    def share_copy(t, d, p, at):
        return remote(
            ybuf.at[1, d, pl.ds(p * PIECE, PIECE), at], hbuf.at[shares + t, pl.ds(d * half + p * PIECE, PIECE), at],
            sb_send.at[d * pieces + p], sb_recv.at[t, p], sib)

    def share_sent(d, p):
        share_copy(0, d, p, pl.ds(0, width)).wait_send()

    def emit(t, d, p):
        @pl.when(t >= 1)
        def _():
            share_sent(d, p)

        def column(i, _):
            at = rows(i * e_tile, e_tile)
            y = jnp.dot(o_s[...], wo[:, at], preferred_element_type=F32).astype(BF16)
            for cc in range(2):
                ybuf[cc + c - 2 * cc * c, d, pl.ds(p * PIECE, PIECE), at] = y[cc * PIECE:(cc + 1) * PIECE]
            share_copy(t, d, p, at).start()
            return 0

        lax.fori_loop(0, width // e_tile, column, 0)

    def sum_copy(s, d, k):
        at = rows(d * half + k * sub, sub)
        return remote(hbuf.at[s, at], hbuf.at[s + 1, at], rs_send.at[k],
                      rs_recv.at[s, k], toward(d) * 2 + c)

    def out_copy(d, k):
        at = rows(d * half + k * sub, sub)
        return pltpu.make_async_copy(hbuf.at[nz - 1, at], out_hbm.at[at], out_sem)

    def add_up(s, k):
        if k * sub % PIECE == 0:
            wait_bytes(hbuf.at[shares + s, pl.ds(0, 2 * PIECE)], sb_recv.at[s, k * sub // PIECE])

        @pl.when(s >= 1)
        def _():
            wait_bytes(hbuf.at[s, pl.ds(0, 2 * sub)], rs_recv.at[s - 1, k])

        for d in range(2):
            at = rows(d * half + k * sub, sub)

            def column(i, _, d=d, at=at):
                lanes = rows(i * y_tile, y_tile)
                y = ybuf[0, d, pl.ds(k * sub, sub), lanes].astype(F32)
                y = y + hbuf[shares + s, at, lanes].astype(F32)
                run = hbuf[s, at, lanes].astype(F32)
                y = (y + jnp.where(s >= 1, run, 0.0)).astype(BF16)
                hbuf[s, at, lanes] = y

                @pl.when(s == nz - 1)
                def _():
                    hbuf[s, at, lanes] = (hbuf[shares, at, lanes].astype(F32) + y.astype(F32)).astype(BF16)

                return 0

            lax.fori_loop(0, width // y_tile, column, 0)

            if d == 0:
                @pl.when(s >= 1)
                def _():
                    sent_bytes(hbuf.at[s - 1, pl.ds(0, 2 * sub)], rs_send.at[k])

            @pl.when(s < nz - 1)
            def _(d=d):
                sum_copy(s, d, k).start()

            @pl.when(s == nz - 1)
            def _(d=d):
                out_copy(d, k).start()

    x_again = pltpu.make_async_copy(x_hbm, hbuf.at[shares], ld_sem.at[0])

    def cache_copy(i, which):
        at = rows(i * cast_rows, cast_rows)
        return pltpu.make_async_copy(
            kv_st.at[which, lax.rem(i, 2)], (k_hbm, v_hbm)[which].at[at], st_sem.at[which, lax.rem(i, 2)])

    def write_caches(i):
        for which in range(2):
            @pl.when(i >= 2)
            def _(which=which):
                cache_copy(i - 2, which).wait()

            part = (k_s, v_s)[which][rows(i * cast_rows, cast_rows), :]
            kv_st[which, lax.rem(i, 2)] = part.reshape(cast_rows, heads, HEAD_DIM)
            cache_copy(i, which).start()

    def scatter_step(t, _):
        @pl.when(t == 2)
        def _():
            x_again.start()

        @pl.when(t == nz)
        def _():
            x_again.wait()

        for k in range(SUM_PIECES):
            @pl.when(t >= 1)
            def _(k=k):
                write_caches((t - 1) * SUM_PIECES + k)
                add_up(t - 1, k)

            d, late = k % 2, k < 2

            @pl.when((t >= 1) if late else (t < nz))
            def _(d=d, late=late):
                attend(t - late, d, int(late))
                emit(t - late, d, int(late))

        return 0

    lax.fori_loop(0, nz + 1, scatter_step, 0)

    for d in range(2):
        for p in range(pieces):
            share_sent(d, p)
    pltpu.make_async_copy(hbuf.at[nz - 1], out_hbm, out_sem).wait()
    for i in (nz * SUM_PIECES - 2, nz * SUM_PIECES - 1):
        for which in range(2):
            cache_copy(i, which).wait()


def flush_kernel(out_ref, k_ref, v_ref, out_hbm, k_hbm, v_hbm, sem):
    copies = []
    for i, (src, dst) in enumerate(((out_ref, out_hbm), (k_ref, k_hbm), (v_ref, v_hbm))):
        part = src.shape[0] // FLUSH_PARTS
        for j in range(FLUSH_PARTS):
            at = pl.ds(j * part, part)
            copies.append(pltpu.make_async_copy(src.at[at], dst.at[at], sem.at[i, j]))
    for copy in copies:
        copy.start()
    for copy in copies:
        copy.wait()


def solution(mesh):
    n = mesh.shape["tp"]

    def local_block(x_local, attn_gain, wq, wk, wv, q_gain, k_gain, wo):
        _, n_rows, width = x_local.shape
        cols = wq.shape[1]
        seq_len = n * n_rows
        nz, pieces = n // 2, n_rows // 2 // PIECE
        units = nz * pieces
        tables = rope_constants(seq_len)
        shapes = ((n_rows, width),) + ((seq_len, cols // HEAD_DIM, HEAD_DIM),) * 2
        any_spec = pl.BlockSpec(memory_space=pl.ANY)
        vmem_spec = pl.BlockSpec(memory_space=pltpu.VMEM)
        dma = pltpu.SemaphoreType.DMA
        held = pl.pallas_call(
            functools.partial(block_kernel, n),
            out_shape=tuple(pltpu.VMEM(shape, BF16) for shape in shapes),
            in_specs=[any_spec, vmem_spec] + [any_spec] * 4 + [vmem_spec] * 6,
            out_specs=(any_spec,) * 3,
            scratch_shapes=[
                pltpu.VMEM((units, 4 * PIECE, width), BF16),
                pltpu.VMEM((3, max(width, seq_len), cols), BF16),
                pltpu.VMEM((cols, width), BF16),
                pltpu.VMEM((seq_len, cols), BF16),
                pltpu.VMEM((seq_len, cols), F32),
                pltpu.VMEM((seq_len, cols), BF16),
                pltpu.VMEM((cols, seq_len), BF16),
                pltpu.VMEM((2, 2, n_rows // 2, width), BF16),
                pltpu.VMEM((2 * PIECE, cols), BF16),
                pltpu.VMEM((2, 2, seq_len // (nz * SUM_PIECES), cols // HEAD_DIM, HEAD_DIM), BF16),
                pltpu.VMEM((units, 2, 2, 2 * PIECE), F32),
                pltpu.VMEM((nz, 2, pieces, 2, 2 * PIECE), F32),
                pltpu.VMEM((n, 2, pieces, 2, 2 * PIECE), F32),
                dma((4 + 2 * pieces,)),
                dma((4,)), dma((units - pieces,)), dma((4,)), dma((units,)),
                dma((4,)), dma, dma, dma((nz,)),
                dma((SUM_PIECES,)), dma((nz - 1, SUM_PIECES)),
                dma((2 * pieces,)), dma((nz, pieces)), dma((2, 2)), dma,
            ],
            compiler_params=pltpu.CompilerParams(
                collective_id=0, has_side_effects=True, vmem_limit_bytes=KERNEL_VMEM),
            name="attention_block",
        )(x_local[0], attn_gain[None], wq, wk, wv, wo, q_gain[None], k_gain[None], *tables)
        out, k_rot, v_rows = pl.pallas_call(
            flush_kernel,
            out_shape=tuple(jax.ShapeDtypeStruct(shape, BF16) for shape in shapes),
            in_specs=[any_spec] * 3, out_specs=(any_spec,) * 3,
            scratch_shapes=[dma((3, FLUSH_PARTS))],
            compiler_params=pltpu.CompilerParams(vmem_limit_bytes=1 << 18),
            name="write_out",
        )(*held)
        return out[None], k_rot[None], v_rows[None]

    seq_spec = P("dp", "tp", None)
    head_spec = P("dp", None, "tp", None)
    col_spec = P(None, "tp")
    return jax.shard_map(
        local_block, mesh=mesh,
        in_specs=(seq_spec, P(None), col_spec, col_spec, col_spec, P("tp"), P("tp"), P("tp", None)),
        out_specs=(seq_spec, head_spec, head_spec), check_vma=False)
```

```python
import functools
import math

import jax
import jax.numpy as jnp
import numpy as np
from jax import lax
from jax.experimental import pallas as pl
from jax.experimental.pallas import tpu as pltpu
from jax.sharding import PartitionSpec as P

HEAD_DIM = 128
EPS = 1e-5
PIECE = 64
SUM_PIECES = 4
KERNEL_VMEM = 60700000
FLUSH_PARTS = 4
F32 = jnp.float32
BF16 = jnp.bfloat16


def rope_constants(seq_len):
    half = HEAD_DIM // 2
    inv_freq = 10000.0 ** (-np.arange(half) * (2.0 / HEAD_DIM))
    inv_freq = np.concatenate([inv_freq, inv_freq])
    sign = np.concatenate([-np.ones(half), np.ones(half)])
    base = (np.arange(seq_len // PIECE) * PIECE)[:, None] * inv_freq
    off = np.arange(PIECE)[:, None] * inv_freq
    return jnp.asarray(np.concatenate([np.cos(base), sign * np.sin(base), np.cos(off), sign * np.sin(off)]), F32)


def block_kernel(
    n, x_hbm, gain_hbm, wq_hbm, wk_hbm, wv_hbm, wo_hbm, q_gain_hbm, k_gain_hbm, turns_hbm,
    out_hbm, k_hbm, v_hbm,
    gain, q_gain, k_gain, turns, hbuf, wqkv, wo, q_s, k_f, v_s, v_t, ybuf, o_s, kv_st, sq_out, sq_in, sums,
    ld_sem, ag_send, ag_recv, dd_send, dd_recv, sq_send, sq_recv, iv_send, iv_recv,
    rs_send, rs_recv, sb_send, sb_recv, st_sem, out_sem,
):
    nz = n // 2
    me = lax.axis_index("tp")
    z, c = me // 2, lax.rem(me, 2)
    sib = z * 2 + 1 - c
    n_rows, width = x_hbm.shape
    half = n_rows // 2
    pieces = half // PIECE
    units = nz * pieces
    cols = q_s.shape[1]
    heads = cols // HEAD_DIM
    sub = half // SUM_PIECES
    k_tile = 2 * n_rows
    shares = units // 2
    cast_rows = q_s.shape[0] // (nz * SUM_PIECES)

    k_s = wqkv.at[0]

    n_base = q_s.shape[0] // PIECE
    starts = (0, n_base, 2 * n_base, 2 * n_base + PIECE)
    cos_b, sin_b, cos_o, sin_o = (
        turns.at[pl.ds(start, size)] for start, size in zip(starts, (n_base, n_base, PIECE, PIECE)))

    def chip(offset):
        return lax.rem(z + offset + 2 * nz, nz)

    def toward(d, hops=1):
        return chip(hops) if d == 0 else chip(-hops)

    def rows(start, size):
        return pl.ds(pl.multiple_of(start, size), size)

    def remote(src, dst, send, recv, dev):
        return pltpu.make_async_remote_copy(
            src_ref=src, dst_ref=dst, send_sem=send, recv_sem=recv,
            device_id={"tp": dev}, device_id_type=pl.DeviceIdType.MESH)

    def wait_bytes(ref, sem):
        remote(ref, ref, sem, sem, sib).wait_recv()

    def x_load(d, p):
        at = pl.ds(d * half + p * PIECE, PIECE)
        return pltpu.make_async_copy(x_hbm.at[at], ybuf.at[0, d, pl.ds(p * PIECE, PIECE)], ld_sem.at[4 + d * pieces + p])

    gain_load = pltpu.make_async_copy(gain_hbm, gain, ld_sem.at[4 + 2 * pieces])
    gain_load.start()
    for p in range(pieces):
        for d in range(2):
            x_load(d, p).start()
    loads = [pltpu.make_async_copy(w, wqkv.at[i, pl.ds(0, width)], ld_sem.at[i]) for i, w in enumerate((wq_hbm, wk_hbm, wv_hbm))]
    loads.append(pltpu.make_async_copy(wo_hbm, wo, ld_sem.at[3]))
    for i, (src, dst) in enumerate(((q_gain_hbm, q_gain), (k_gain_hbm, k_gain), (turns_hbm, turns))):
        loads.append(pltpu.make_async_copy(src, dst, ld_sem.at[5 + 2 * pieces + i]))

    barrier = pltpu.get_barrier_semaphore()

    for dev in (sib, toward(0) * 2 + c, toward(1) * 2 + c):
        pl.semaphore_signal(barrier, inc=1, device_id={"tp": dev}, device_id_type=pl.DeviceIdType.MESH)

    def quarter(u, d):
        return hbuf.at[u, rows((2 * d + c) * PIECE, PIECE)]

    def ring_copy(u, d):
        return remote(quarter(u, d), quarter(u + pieces, d), ag_send.at[lax.rem(u, 4)], ag_recv.at[u], toward(d) * 2 + c)

    def pair_copy(u, d):
        return remote(quarter(u, d), quarter(u, d), dd_send.at[lax.rem(u, 4)], dd_recv.at[u], sib)

    gain_load.wait()
    for p in range(pieces):
        for d in range(2):
            x_load(d, p).wait()
            x = ybuf[0, d, pl.ds(p * PIECE, PIECE), :].astype(F32)
            inv_rms = lax.rsqrt(jnp.mean(x * x, axis=-1, keepdims=True) + EPS)
            hbuf[p, rows((2 * d + c) * PIECE, PIECE), :] = (x * inv_rms * gain[...]).astype(BF16)
        if p == 0:
            for load in loads:
                load.start()
            pl.semaphore_wait(barrier, 3)
        for d in range(2):
            ring_copy(p, d).start()
            pair_copy(p, d).start()

    def sq_copy(u, d, p, dev):
        return remote(sq_out.at[u, d], sq_in.at[z, d, p], sq_send.at[lax.rem(u, 4)], sq_recv, dev)

    def rotate(t, src, d, cc, p):
        b = (2 * src + cc) * (n_rows // PIECE) + d * pieces + p
        cb, sb = cos_b[pl.ds(b, 1), :], sin_b[pl.ds(b, 1), :]
        cos = cb * cos_o[...] - sb * sin_o[...]
        sin = sb * cos_o[...] + cb * sin_o[...]
        heads_in = [t[:, j * HEAD_DIM:(j + 1) * HEAD_DIM] for j in range(heads)]
        return [x * cos + pltpu.roll(x, HEAD_DIM // 2, 1) * sin for x in heads_in]

    def project(v):
        s, p = v // pieces, lax.rem(v, pieces)
        wait_bytes(hbuf.at[v, pl.ds(0, 2 * PIECE)], dd_recv.at[v])

        @pl.when(v == 0)
        def _():
            for load in loads:
                load.wait()

        h = hbuf[v]
        parts = [(d, cc, chip(-s) if d == 0 else chip(s), (2 * d + cc) * PIECE) for d in range(2) for cc in range(2)]

        def at(d, cc, src):
            return rows((2 * src + cc) * n_rows + d * half + p * PIECE, PIECE)

        outs, squares = [], []
        for i in range(2):
            out = jnp.dot(h, wqkv[i, :width], preferred_element_type=F32).astype(BF16)
            wide = out.astype(F32)
            sq = wide * wide
            lanes = sq[:, :HEAD_DIM]
            for j in range(1, heads):
                lanes = lanes + sq[:, j * HEAD_DIM:(j + 1) * HEAD_DIM]
            outs.append(out)
            squares.append(lanes)
        for d in range(2):
            for i in range(2):
                part = squares[i][d * 2 * PIECE:(d + 1) * 2 * PIECE]
                sq_out[v, d, pl.ds(i, 1), :] = jnp.sum(part.T, axis=0, keepdims=True)
            owner = chip(-s - 1) if d == 0 else chip(s + 1)

            @pl.when(s < nz - 1)
            def _(d=d, owner=owner):
                sq_copy(v, d, p, owner * 2 + c).start()

            @pl.when(s == nz - 1)
            def _(d=d):
                sq_in[z, d, p] = sq_out[v, d]

        for d, cc, src, lo in parts:
            q_s[at(d, cc, src), :] = outs[0][lo:lo + PIECE]
            k_f[at(d, cc, src), :] = outs[1][lo:lo + PIECE].astype(F32)

    def project_rest(v):
        s, p = v // pieces, lax.rem(v, pieces)
        out = jnp.dot(hbuf[v], wqkv[2, :width], preferred_element_type=F32).astype(BF16)
        for d in range(2):
            src = chip(-s) if d == 0 else chip(s)
            for cc in range(2):
                at = rows((2 * src + cc) * n_rows + d * half + p * PIECE, PIECE)
                lo = (2 * d + cc) * PIECE
                v_s[at, :] = out[lo:lo + PIECE]
                done = rotate(k_f[at, :] * k_gain[...], src, d, cc, p)
                for j in range(heads):
                    k_f[at, j * HEAD_DIM:(j + 1) * HEAD_DIM] = done[j]

    def sent_bytes(ref, sem):
        remote(ref, ref, sem, sem, sib).wait_send()

    def drain(u):
        both = hbuf.at[u, pl.ds(0, 2 * PIECE)]
        sent_bytes(both, dd_send.at[lax.rem(u, 4)])

        @pl.when(u < units - pieces)
        def _():
            sent_bytes(both, ag_send.at[lax.rem(u, 4)])
            sent_bytes(sq_out.at[u], sq_send.at[lax.rem(u, 4)])

    def gather_step(u, _):
        @pl.when(u >= pieces)
        def _():
            wait_bytes(hbuf.at[u, pl.ds(0, 2 * PIECE)], ag_recv.at[u - pieces])
            for d in range(2):
                @pl.when(u < units - pieces)
                def _(d=d):
                    ring_copy(u, d).start()

                pair_copy(u, d).start()

        project(u)

        @pl.when(u >= 2)
        def _():
            drain(u - 2)

        @pl.when(u < units - 1)
        def _():
            project_rest(u)

        return 0

    lax.fori_loop(0, units, gather_step, 0)
    drain(units - 2)
    drain(units - 1)

    wait_bytes(sq_in.at[pl.ds(0, nz - 1)], sq_recv)
    total = sq_in[0]
    for i in range(1, nz):
        total = total + sq_in[i]
    sums[me] = total

    def inv_start(i, _):
        dev = lax.rem(me + n // 2 + i // 2 * (1 - 2 * lax.rem(i, 2)) + n, n)
        remote(sums.at[me], sums.at[me], iv_send, iv_recv.at[z], dev).start()
        return 0

    def sums_of(offset):
        at = sums.at[pl.ds(0, 1 if offset == 0 else 2)]
        wait_bytes(at, iv_recv.at[chip(offset)])

    lax.fori_loop(1, n, inv_start, 0)
    project_rest(units - 1)

    def turn_values(i, _):
        at = rows(i * k_tile, k_tile)
        v_t[:, at] = v_s[at, :].T
        return 0

    lax.fori_loop(0, q_s.shape[0] // k_tile, turn_values, 0)
    def row_scale(which, src, d, p):
        own = lax.rem(src + (nz - 1 if d == 0 else 1), nz) * 2
        total = sums[own, d, p][which:which + 1] + sums[own + 1, d, p][which:which + 1]
        return jnp.broadcast_to(lax.rsqrt(total / (cols * n) + EPS), (HEAD_DIM, HEAD_DIM)).T

    def piece_rows(src, cc, d, p):
        return rows((2 * src + cc) * n_rows + d * half + p * PIECE, PIECE)

    def finish_keys(src):
        for d in range(2):
            for p in range(pieces):
                scale = row_scale(1, src, d, p)
                for cc in range(2):
                    at = piece_rows(src, cc, d, p)
                    for j in range(heads):
                        lanes = slice(j * HEAD_DIM, (j + 1) * HEAD_DIM)
                        k_s[at, lanes] = (k_f[at, lanes] * scale[cc * PIECE:(cc + 1) * PIECE]).astype(BF16)

    def finish_near(distance):
        for offset in sorted({distance, -distance % nz}):
            finish_keys(chip(offset))

    sums_of(0)
    for distance in range(1, nz // 2 + 1):
        for offset in sorted({distance, -distance % nz}):
            sums_of(offset)
        finish_near(distance - 1)
        if distance == nz // 2 - 1:
            finish_near(nz // 2)
    others = sums.at[pl.ds(0, n - 1)]
    sent_bytes(others, iv_send)

    scale = HEAD_DIM ** -0.5 * math.log2(math.e)

    queries = 2 * PIECE

    def attend(t, d, p):
        blk = lax.rem(z + 2 * nz - 1 - t, nz) if d == 0 else lax.rem(z + 1 + t, nz)
        factor = row_scale(0, blk, d, p)
        factor = jnp.concatenate([factor] * heads, axis=1)
        parts = []
        for cc in range(2):
            raw = q_s[piece_rows(blk, cc, d, p), :].astype(F32)
            parts.append(rotate(raw * factor[cc * PIECE:(cc + 1) * PIECE] * q_gain[...], blk, d, cc, p))
        q_t = [jnp.concatenate([parts[0][j], parts[1][j]], axis=0).T.astype(BF16) for j in range(heads)]

        head = [slice(j * HEAD_DIM, (j + 1) * HEAD_DIM) for j in range(heads)]

        def scores(at):
            return [jnp.dot(k_s[at, head[j]], q_t[j], preferred_element_type=F32) for j in range(heads)]

        def update(at, score, carry):
            peak = [jnp.maximum(carry[j][0], jnp.max(score[j], axis=0, keepdims=True)) for j in range(heads)]
            prob = [jnp.exp2(score[j] * scale - peak[j] * scale) for j in range(heads)]
            fade = [jnp.exp2((carry[j][0] - peak[j]) * scale) for j in range(heads)]
            acc = [jnp.dot(v_t[head[j], at], prob[j].astype(BF16), preferred_element_type=F32) for j in range(heads)]
            return tuple(
                (peak[j], carry[j][1] * fade[j] + jnp.sum(prob[j], axis=0, keepdims=True), carry[j][2] * fade[j] + acc[j])
                for j in range(heads))

        def one(i, carry):
            at = rows(i * k_tile, k_tile)
            return update(at, scores(at), carry)

        def two(i, carry):
            at = [rows((2 * i + m) * k_tile, k_tile) for m in range(2)]
            both = [scores(a) for a in at]
            return update(at[1], both[1], update(at[0], both[0], carry))

        zero = (jnp.full((1, queries), -1e30, F32), jnp.zeros((1, queries), F32), jnp.zeros((HEAD_DIM, queries), F32))
        pairs = blk // 2
        carry = lax.fori_loop(0, pairs, two, (zero,) * heads)
        carry = lax.fori_loop(2 * pairs, blk, one, carry)
        key = lax.broadcasted_iota(jnp.int32, (k_tile, queries), 0)
        r = lax.broadcasted_iota(jnp.int32, (k_tile, queries), 1)
        mask = jnp.where(r < PIECE, r, r + (n_rows - PIECE)) + (d * half + p * PIECE) >= key
        at = rows(blk * k_tile, k_tile)
        carry = update(at, [jnp.where(mask, sc, -1e30) for sc in scores(at)], carry)
        for j in range(heads):
            _, l, acc = carry[j]
            o_s[:, j * HEAD_DIM:(j + 1) * HEAD_DIM] = (acc / l).T.astype(BF16)

    y_tile, e_tile = min(width, 1024), min(width, 2048)

    def share_copy(t, d, p, at):
        return remote(
            ybuf.at[1, d, pl.ds(p * PIECE, PIECE), at], hbuf.at[shares + t, pl.ds(d * half + p * PIECE, PIECE), at],
            sb_send.at[d * pieces + p], sb_recv.at[t, p], sib)

    def share_sent(d, p):
        share_copy(0, d, p, pl.ds(0, width)).wait_send()

    def emit(t, d, p):
        @pl.when(t >= 1)
        def _():
            share_sent(d, p)

        def column(i, _):
            at = rows(i * e_tile, e_tile)
            y = jnp.dot(o_s[...], wo[:, at], preferred_element_type=F32).astype(BF16)
            for cc in range(2):
                ybuf[cc + c - 2 * cc * c, d, pl.ds(p * PIECE, PIECE), at] = y[cc * PIECE:(cc + 1) * PIECE]
            share_copy(t, d, p, at).start()
            return 0

        lax.fori_loop(0, width // e_tile, column, 0)

    def sum_copy(s, d, k):
        at = rows(d * half + k * sub, sub)
        return remote(hbuf.at[s, at], hbuf.at[s + 1, at], rs_send.at[k],
                      rs_recv.at[s, k], toward(d) * 2 + c)

    def out_copy(d, k):
        at = rows(d * half + k * sub, sub)
        return pltpu.make_async_copy(hbuf.at[nz - 1, at], out_hbm.at[at], out_sem)

    def add_up(s, k):
        if k * sub % PIECE == 0:
            wait_bytes(hbuf.at[shares + s, pl.ds(0, 2 * PIECE)], sb_recv.at[s, k * sub // PIECE])

        @pl.when(s >= 1)
        def _():
            wait_bytes(hbuf.at[s, pl.ds(0, 2 * sub)], rs_recv.at[s - 1, k])

        for d in range(2):
            at = rows(d * half + k * sub, sub)

            def column(i, _, d=d, at=at):
                lanes = rows(i * y_tile, y_tile)
                y = ybuf[0, d, pl.ds(k * sub, sub), lanes].astype(F32)
                y = y + hbuf[shares + s, at, lanes].astype(F32)
                run = hbuf[s, at, lanes].astype(F32)
                y = (y + jnp.where(s >= 1, run, 0.0)).astype(BF16)
                hbuf[s, at, lanes] = y

                @pl.when(s == nz - 1)
                def _():
                    hbuf[s, at, lanes] = (hbuf[shares, at, lanes].astype(F32) + y.astype(F32)).astype(BF16)

                return 0

            lax.fori_loop(0, width // y_tile, column, 0)

            if d == 0:
                @pl.when(s >= 1)
                def _():
                    sent_bytes(hbuf.at[s - 1, pl.ds(0, 2 * sub)], rs_send.at[k])

            @pl.when(s < nz - 1)
            def _(d=d):
                sum_copy(s, d, k).start()

            @pl.when(s == nz - 1)
            def _(d=d):
                out_copy(d, k).start()

    x_again = pltpu.make_async_copy(x_hbm, hbuf.at[shares], ld_sem.at[0])

    def cache_copy(i, which):
        at = rows(i * cast_rows, cast_rows)
        return pltpu.make_async_copy(
            kv_st.at[which, lax.rem(i, 2)], (k_hbm, v_hbm)[which].at[at], st_sem.at[which, lax.rem(i, 2)])

    def write_caches(i):
        for which in range(2):
            @pl.when(i >= 2)
            def _(which=which):
                cache_copy(i - 2, which).wait()

            part = (k_s, v_s)[which][rows(i * cast_rows, cast_rows), :]
            kv_st[which, lax.rem(i, 2)] = part.reshape(cast_rows, heads, HEAD_DIM)
            cache_copy(i, which).start()

    def scatter_step(t, _):
        @pl.when(t == 2)
        def _():
            x_again.start()

        @pl.when(t == nz)
        def _():
            x_again.wait()

        for k in range(SUM_PIECES):
            @pl.when(t >= 1)
            def _(k=k):
                write_caches((t - 1) * SUM_PIECES + k)
                add_up(t - 1, k)

            d, late = k % 2, k < 2

            @pl.when((t >= 1) if late else (t < nz))
            def _(d=d, late=late):
                attend(t - late, d, int(late))
                emit(t - late, d, int(late))

        return 0

    lax.fori_loop(0, nz + 1, scatter_step, 0)

    for d in range(2):
        for p in range(pieces):
            share_sent(d, p)
    pltpu.make_async_copy(hbuf.at[nz - 1], out_hbm, out_sem).wait()
    for i in (nz * SUM_PIECES - 2, nz * SUM_PIECES - 1):
        for which in range(2):
            cache_copy(i, which).wait()


def flush_kernel(out_ref, k_ref, v_ref, out_hbm, k_hbm, v_hbm, sem):
    copies = []
    for i, (src, dst) in enumerate(((out_ref, out_hbm), (k_ref, k_hbm), (v_ref, v_hbm))):
        part = src.shape[0] // FLUSH_PARTS
        for j in range(FLUSH_PARTS):
            at = pl.ds(j * part, part)
            copies.append(pltpu.make_async_copy(src.at[at], dst.at[at], sem.at[i, j]))
    for copy in copies:
        copy.start()
    for copy in copies:
        copy.wait()


def solution(mesh):
    n = mesh.shape["tp"]

    def local_block(x_local, attn_gain, wq, wk, wv, q_gain, k_gain, wo):
        _, n_rows, width = x_local.shape
        cols = wq.shape[1]
        seq_len = n * n_rows
        nz, pieces = n // 2, n_rows // 2 // PIECE
        units = nz * pieces
        turns = rope_constants(seq_len)
        shapes = ((n_rows, width),) + ((seq_len, cols // HEAD_DIM, HEAD_DIM),) * 2
        any_spec = pl.BlockSpec(memory_space=pl.ANY)
        dma = pltpu.SemaphoreType.DMA
        held = pl.pallas_call(
            functools.partial(block_kernel, n),
            out_shape=tuple(pltpu.VMEM(shape, BF16) for shape in shapes),
            in_specs=[any_spec] * 9,
            out_specs=(any_spec,) * 3,
            scratch_shapes=[
                pltpu.VMEM((1, width), F32),
                pltpu.VMEM((1, cols), F32),
                pltpu.VMEM((1, cols), F32),
                pltpu.VMEM(turns.shape, F32),
                pltpu.VMEM((units, 4 * PIECE, width), BF16),
                pltpu.VMEM((3, max(width, seq_len), cols), BF16),
                pltpu.VMEM((cols, width), BF16),
                pltpu.VMEM((seq_len, cols), BF16),
                pltpu.VMEM((seq_len, cols), F32),
                pltpu.VMEM((seq_len, cols), BF16),
                pltpu.VMEM((cols, seq_len), BF16),
                pltpu.VMEM((2, 2, n_rows // 2, width), BF16),
                pltpu.VMEM((2 * PIECE, cols), BF16),
                pltpu.VMEM((2, 2, seq_len // (nz * SUM_PIECES), cols // HEAD_DIM, HEAD_DIM), BF16),
                pltpu.VMEM((units, 2, 2, 2 * PIECE), F32),
                pltpu.VMEM((nz, 2, pieces, 2, 2 * PIECE), F32),
                pltpu.VMEM((n, 2, pieces, 2, 2 * PIECE), F32),
                dma((8 + 2 * pieces,)),
                dma((4,)), dma((units - pieces,)), dma((4,)), dma((units,)),
                dma((4,)), dma, dma, dma((nz,)),
                dma((SUM_PIECES,)), dma((nz - 1, SUM_PIECES)),
                dma((2 * pieces,)), dma((nz, pieces)), dma((2, 2)), dma,
            ],
            compiler_params=pltpu.CompilerParams(
                collective_id=0, has_side_effects=True, vmem_limit_bytes=KERNEL_VMEM),
            name="attention_block",
        )(x_local[0], attn_gain[None], wq, wk, wv, wo, q_gain[None], k_gain[None], turns)
        out, k_rot, v_rows = pl.pallas_call(
            flush_kernel,
            out_shape=tuple(jax.ShapeDtypeStruct(shape, BF16) for shape in shapes),
            in_specs=[any_spec] * 3, out_specs=(any_spec,) * 3,
            scratch_shapes=[dma((3, FLUSH_PARTS))],
            compiler_params=pltpu.CompilerParams(vmem_limit_bytes=1 << 18),
            name="write_out",
        )(*held)
        return out[None], k_rot[None], v_rows[None]

    seq_spec = P("dp", "tp", None)
    head_spec = P("dp", None, "tp", None)
    col_spec = P(None, "tp")
    return jax.shard_map(
        local_block, mesh=mesh,
        in_specs=(seq_spec, P(None), col_spec, col_spec, col_spec, P("tp"), P("tp"), P("tp", None)),
        out_specs=(seq_spec, head_spec, head_spec), check_vma=False)
```
